32 devices in a mesh: dp: 1 (over z), ep: 32 (over y, x, core).
Axes of the slice: x: 4, y: 4, z: 1, core: 2. Of those that a mesh axis runs over, the one named last changes fastest.
The devices are a block of a 4x4x8 slice.
Arguments:
- hidden_in: bfloat16 [1024, 2048], P(('dp', 'ep'))
- kv_cache: bfloat16 [1024, 256, 576], P(('dp', 'ep'))
- kv_lens: int32 [1024], P(('dp', 'ep'))
- routes: int32 [1024, 6], P(('dp', 'ep'))
- route_gates: float32 [1024, 6], P(('dp', 'ep'))
- w_q: bfloat16 [2048, 3072], replicated
- w_dkv: bfloat16 [2048, 576], replicated
- w_uk: bfloat16 [16, 128, 512], replicated
- w_uv: bfloat16 [16, 512, 128], replicated
- w_o: bfloat16 [2048, 2048], replicated
- sh_gate: bfloat16 [2048, 2816], replicated
- sh_up: bfloat16 [2048, 2816], replicated
- sh_down: bfloat16 [2816, 2048], replicated
- ex_gate: bfloat16 [64, 2048, 1408], P('ep')
- ex_up: bfloat16 [64, 2048, 1408], P('ep')
- ex_down: bfloat16 [64, 1408, 2048], P('ep')
Outputs:
- output 1: bfloat16 [1024, 2048], P(('dp', 'ep'))
- output 2: bfloat16 [1024, 576], P(('dp', 'ep'))
All inputs are finite; a program needn't handle non-finite values.
Results may differ from the reference program's by a relative error of at most 0.0158559.
Values are sent between devices in bfloat16 or wider.
A program may use at most 768 MiB of HBM per device.

```python
import jax
import jax.numpy as jnp
from jax import lax

HIDDEN = 2048
NUM_HEADS = 16
NOPE_DIM = 128
ROPE_DIM = 64
V_DIM = 128
LATENT = 512
EXPERTS = 64
TOP_K = 6
MOE_FF = 1408
SHARED_FF = 2816
SEQS_DEV = 32
CACHE_LEN = 256
GROUP_SIZE = 32


def draw_lengths(rng_key):
    key_dev, key_seq, key_top = jax.random.split(rng_key, 3)
    key_shift, key_mant = jax.random.split(key_dev)
    num_seq = GROUP_SIZE * SEQS_DEV
    dev_shift = jax.random.randint(key_shift, (GROUP_SIZE, 1), 1, 5, jnp.int32)
    dev_mant = jax.random.randint(key_mant, (GROUP_SIZE, 1), 0, 256, jnp.int32)
    dev_num = (256 + dev_mant) >> dev_shift
    seq_draw = jax.random.randint(key_seq, (GROUP_SIZE, SEQS_DEV), 0, CACHE_LEN, jnp.int32)
    lengths = ((dev_num * seq_draw) >> 8).astype(jnp.int32).reshape(num_seq)
    lengths = jnp.minimum(lengths, CACHE_LEN - 1)
    top_pos = jax.random.randint(key_top, (), 0, num_seq)
    return jnp.where(jnp.arange(num_seq) == top_pos, CACHE_LEN - 1, lengths).astype(jnp.int32)


def draw_routes(rng_key):
    n_hot = GROUP_SIZE // 4
    n_cold = GROUP_SIZE - n_hot
    hot_picks = (3 * TOP_K) // 4
    local_exp = EXPERTS // GROUP_SIZE
    key_perm, key_hot, key_cold, key_exp, key_order = jax.random.split(rng_key, 5)
    dev_order = jax.random.permutation(key_perm, GROUP_SIZE)
    exp_shift = jax.random.randint(key_exp, (GROUP_SIZE, GROUP_SIZE), 0, local_exp)
    src_dev = jnp.arange(GROUP_SIZE)[:, None]

    def pick_experts(dev_list, dev_count, per_token, shift_key):
        pos_shift = jax.random.randint(shift_key, (GROUP_SIZE, 1), 0, dev_count)
        copy_pos = jnp.arange(SEQS_DEV * per_token)[None, :] + pos_shift
        dst_dev = dev_list[copy_pos % dev_count]
        local_id = (copy_pos // dev_count + exp_shift[src_dev, dst_dev]) % local_exp
        return (dst_dev * local_exp + local_id).reshape(GROUP_SIZE, SEQS_DEV, per_token)

    hot_ids = pick_experts(dev_order[:n_hot], n_hot, hot_picks, key_hot)
    cold_ids = pick_experts(dev_order[n_hot:], n_cold, TOP_K - hot_picks, key_cold)
    all_ids = jnp.concatenate([hot_ids, cold_ids], axis=2).reshape(GROUP_SIZE * SEQS_DEV, TOP_K)
    col_order = jnp.argsort(jax.random.uniform(key_order, (GROUP_SIZE * SEQS_DEV, TOP_K), jnp.float32), axis=1)
    return jnp.take_along_axis(all_ids, col_order, axis=1).astype(jnp.int32)


def setup_inputs(seed: int = 0, part: int = 0) -> dict:
    base_key = jax.random.key(seed)
    part_keys = jax.random.split(jax.random.fold_in(base_key, part), 5)
    weight_keys = jax.random.split(base_key, 11)
    num_seq = GROUP_SIZE * SEQS_DEV
    lat_row = LATENT + ROPE_DIM

    def normal_w(rng_key, shape_w, fan_in, gain_mul):
        return (jax.random.normal(rng_key, shape_w, jnp.float32) * (gain_mul * fan_in ** -0.5)).astype(jnp.bfloat16)

    return {
        "hidden_in": jax.random.normal(part_keys[0], (num_seq, HIDDEN), jnp.float32).astype(jnp.bfloat16),
        "kv_cache": jax.random.normal(part_keys[1], (num_seq, CACHE_LEN, lat_row), jnp.float32).astype(jnp.bfloat16),
        "kv_lens": draw_lengths(part_keys[2]),
        "routes": draw_routes(part_keys[3]),
        "route_gates": jax.nn.softmax(0.7 * jax.random.normal(part_keys[4], (num_seq, TOP_K), jnp.float32), axis=-1),
        "w_q": normal_w(weight_keys[0], (HIDDEN, NUM_HEADS * (NOPE_DIM + ROPE_DIM)), HIDDEN, 1.0),
        "w_dkv": normal_w(weight_keys[1], (HIDDEN, lat_row), HIDDEN, 1.0),
        "w_uk": normal_w(weight_keys[2], (NUM_HEADS, NOPE_DIM, LATENT), NOPE_DIM, 1.0),
        "w_uv": normal_w(weight_keys[3], (NUM_HEADS, LATENT, V_DIM), LATENT, 3.0),
        "w_o": normal_w(weight_keys[4], (NUM_HEADS * V_DIM, HIDDEN), NUM_HEADS * V_DIM, 1.0),
        "sh_gate": normal_w(weight_keys[5], (HIDDEN, SHARED_FF), HIDDEN, 1.0),
        "sh_up": normal_w(weight_keys[6], (HIDDEN, SHARED_FF), HIDDEN, 1.0),
        "sh_down": normal_w(weight_keys[7], (SHARED_FF, HIDDEN), SHARED_FF, 1.0),
        "ex_gate": normal_w(weight_keys[8], (EXPERTS, HIDDEN, MOE_FF), HIDDEN, 1.0),
        "ex_up": normal_w(weight_keys[9], (EXPERTS, HIDDEN, MOE_FF), HIDDEN, 1.0),
        "ex_down": normal_w(weight_keys[10], (EXPERTS, MOE_FF, HIDDEN), MOE_FF, 1.0),
    }


def rotary(vec, cos_t, sin_t):
    half_dim = vec.shape[-1] // 2
    lead_part = vec[..., :half_dim]
    tail_part = vec[..., half_dim:]
    return jnp.concatenate([lead_part * cos_t - tail_part * sin_t, tail_part * cos_t + lead_part * sin_t], axis=-1)


def rotary_table(positions, rot_width):
    half_dim = rot_width // 2
    inv_freq = jnp.exp(jnp.arange(half_dim, dtype=jnp.float32) * (-2.0 * jnp.log(10000.0) / rot_width))
    angle_val = positions.astype(jnp.float32)[:, None] * inv_freq[None, :]
    return jnp.cos(angle_val), jnp.sin(angle_val)


def swiglu(rows_in, w_gate, w_up, w_down):
    gate_val = jnp.dot(rows_in, w_gate, preferred_element_type=jnp.float32)
    up_val = jnp.dot(rows_in, w_up, preferred_element_type=jnp.float32)
    act_val = (jax.nn.silu(gate_val) * up_val).astype(jnp.bfloat16)
    return jnp.dot(act_val, w_down, preferred_element_type=jnp.float32).astype(jnp.bfloat16)


def attend_block(x_blk, cache_blk, len_blk, w_q, w_dkv, w_uk, w_uv, w_o):
    num_seq = x_blk.shape[0]
    q_all = jnp.dot(x_blk, w_q, preferred_element_type=jnp.float32).astype(jnp.bfloat16)
    q_all = q_all.reshape(num_seq, NUM_HEADS, NOPE_DIM + ROPE_DIM)
    kv_raw = jnp.dot(x_blk, w_dkv, preferred_element_type=jnp.float32)
    cos_t, sin_t = rotary_table(len_blk, ROPE_DIM)
    kv_row = jnp.concatenate([kv_raw[:, :LATENT], rotary(kv_raw[:, LATENT:], cos_t, sin_t)], axis=1).astype(jnp.bfloat16)
    q_rope = rotary(q_all[:, :, NOPE_DIM:].astype(jnp.float32), cos_t[:, None, :], sin_t[:, None, :]).astype(jnp.bfloat16)
    q_lat = jnp.einsum("bhn,hnc->bhc", q_all[:, :, :NOPE_DIM].astype(jnp.float32), w_uk.astype(jnp.float32)).astype(jnp.bfloat16)
    q_cat = jnp.concatenate([q_lat, q_rope], axis=2).astype(jnp.float32)
    score_scale = (NOPE_DIM + ROPE_DIM) ** -0.5
    cache_wide = cache_blk.astype(jnp.float32)
    kv_wide = kv_row.astype(jnp.float32)
    s_old = jnp.einsum("bhc,blc->bhl", q_cat, cache_wide) * score_scale
    s_new = jnp.einsum("bhc,bc->bh", q_cat, kv_wide) * score_scale
    valid_mask = jnp.arange(CACHE_LEN)[None, None, :] < len_blk[:, None, None]
    s_old = jnp.where(valid_mask, s_old, -jnp.inf)
    top_score = jnp.maximum(jnp.max(s_old, axis=2), s_new)
    e_old = jnp.exp(s_old - top_score[:, :, None])
    e_new = jnp.exp(s_new - top_score)
    denom_sum = jnp.sum(e_old, axis=2) + e_new
    p_old = (e_old / denom_sum[:, :, None]).astype(jnp.bfloat16).astype(jnp.float32)
    p_new = (e_new / denom_sum).astype(jnp.bfloat16).astype(jnp.float32)
    o_full = jnp.einsum("bhl,blc->bhc", p_old, cache_wide) + p_new[:, :, None] * kv_wide[:, None, :]
    o_lat = o_full[:, :, :LATENT].astype(jnp.bfloat16)
    v_head = jnp.einsum("bhc,hcv->bhv", o_lat.astype(jnp.float32), w_uv.astype(jnp.float32)).astype(jnp.bfloat16)
    attn_out = jnp.dot(v_head.reshape(num_seq, NUM_HEADS * V_DIM), w_o, preferred_element_type=jnp.float32).astype(jnp.bfloat16)
    h_mid = (x_blk.astype(jnp.float32) + attn_out.astype(jnp.float32)).astype(jnp.bfloat16)
    return h_mid, kv_row


def reference(hidden_in, kv_cache, kv_lens, routes, route_gates, w_q, w_dkv, w_uk, w_uv, w_o, sh_gate, sh_up, sh_down, ex_gate, ex_up, ex_down):
    num_seq = GROUP_SIZE * SEQS_DEV
    lat_row = LATENT + ROPE_DIM

    def per_device(dev_blocks):
        return attend_block(dev_blocks[0], dev_blocks[1], dev_blocks[2], w_q, w_dkv, w_uk, w_uv, w_o)

    h_mid, kv_row = lax.map(per_device, (hidden_in.reshape(GROUP_SIZE, SEQS_DEV, HIDDEN), kv_cache.reshape(GROUP_SIZE, SEQS_DEV, CACHE_LEN, lat_row), kv_lens.reshape(GROUP_SIZE, SEQS_DEV)))
    h_mid = h_mid.reshape(num_seq, HIDDEN)
    kv_row = kv_row.reshape(num_seq, lat_row)
    shared = swiglu(h_mid, sh_gate, sh_up, sh_down)
    local_exp = EXPERTS // GROUP_SIZE
    hot_devs = GROUP_SIZE // 4
    pair_cap = (SEQS_DEV * ((3 * TOP_K) // 4) + hot_devs - 1) // hot_devs
    exp_cap = (pair_cap + local_exp - 1) // local_exp
    rows_per_exp = GROUP_SIZE * exp_cap
    ids_dev = routes.reshape(GROUP_SIZE, SEQS_DEV * TOP_K)
    onehot = (ids_dev[:, :, None] == jnp.arange(EXPERTS)[None, None, :]).astype(jnp.int32)
    rank_pos = jnp.sum((jnp.cumsum(onehot, axis=1) - onehot) * onehot, axis=2)
    row_pos = (ids_dev * rows_per_exp + jnp.arange(GROUP_SIZE)[:, None] * exp_cap + rank_pos).reshape(-1)
    token_ids = jnp.arange(num_seq * TOP_K) // TOP_K
    table_tok = jnp.zeros((EXPERTS * rows_per_exp,), jnp.int32).at[row_pos].set(token_ids)
    table_gate = jnp.zeros((EXPERTS * rows_per_exp,), jnp.float32).at[row_pos].set(route_gates.reshape(-1))

    def add_expert(routed_acc, per_exp):
        exp_tok = per_exp[3]
        exp_out = swiglu(jnp.take(h_mid, exp_tok, axis=0), per_exp[0], per_exp[1], per_exp[2])
        routed_acc = routed_acc + jax.ops.segment_sum(exp_out.astype(jnp.float32) * per_exp[4][:, None], exp_tok, num_segments=num_seq)
        return routed_acc, None

    routed = lax.scan(add_expert, jnp.zeros((num_seq, HIDDEN), jnp.float32), (ex_gate, ex_up, ex_down, table_tok.reshape(EXPERTS, rows_per_exp), table_gate.reshape(EXPERTS, rows_per_exp)))[0]
    layer_out = (h_mid.astype(jnp.float32) + shared.astype(jnp.float32) + routed).astype(jnp.bfloat16)
    return (layer_out, kv_row)
```

```python
import functools

import jax
import jax.numpy as jnp
from jax import lax
from jax.experimental import pallas as pl
from jax.experimental.pallas import tpu as pltpu
from jax.sharding import PartitionSpec as P

MESH = pl.DeviceIdType.MESH
SLOTS_EXP = 8
LANES = 128

def rotary(vec, cos_t, sin_t):
    half_dim = vec.shape[-1] // 2
    lead_part = vec[..., :half_dim]
    tail_part = vec[..., half_dim:]
    return jnp.concatenate([lead_part * cos_t - tail_part * sin_t, tail_part * cos_t + lead_part * sin_t], axis=-1)


def rotary_table(positions, rot_width):
    half_dim = rot_width // 2
    inv_freq = jnp.exp(jnp.arange(half_dim, dtype=jnp.float32) * (-2.0 * jnp.log(10000.0) / rot_width))
    angle_val = positions.astype(jnp.float32)[:, None] * inv_freq[None, :]
    return jnp.cos(angle_val), jnp.sin(angle_val)


def attend_local(x_blk, cache_blk, len_blk, w_q, w_dkv, w_uk, w_uv, w_o):
    num_seq = x_blk.shape[0]
    num_heads, nope_dim, latent = w_uk.shape
    rope_dim = cache_blk.shape[2] - latent
    v_dim = w_uv.shape[2]
    q_all = jnp.dot(x_blk, w_q, preferred_element_type=jnp.float32).astype(jnp.bfloat16).reshape(num_seq, num_heads, nope_dim + rope_dim)
    kv_raw = jnp.dot(x_blk, w_dkv, preferred_element_type=jnp.float32)
    cos_t, sin_t = rotary_table(len_blk, rope_dim)
    kv_row = jnp.concatenate([kv_raw[:, :latent], rotary(kv_raw[:, latent:], cos_t, sin_t)], axis=1).astype(jnp.bfloat16)
    q_rope = rotary(q_all[:, :, nope_dim:].astype(jnp.float32), cos_t[:, None, :], sin_t[:, None, :]).astype(jnp.bfloat16)
    q_lat = jnp.einsum("bhn,hnc->bhc", q_all[:, :, :nope_dim], w_uk, preferred_element_type=jnp.float32).astype(jnp.bfloat16)
    q_cat = jnp.concatenate([q_lat, q_rope], axis=2)
    score_scale = (nope_dim + rope_dim) ** -0.5
    s_old = jnp.einsum("bhc,blc->bhl", q_cat, cache_blk, preferred_element_type=jnp.float32) * score_scale
    s_new = jnp.einsum("bhc,bc->bh", q_cat, kv_row, preferred_element_type=jnp.float32) * score_scale
    valid_mask = jnp.arange(cache_blk.shape[1])[None, None, :] < len_blk[:, None, None]
    s_old = jnp.where(valid_mask, s_old, -jnp.inf)
    top_score = jnp.maximum(jnp.max(s_old, axis=2), s_new)
    e_old = jnp.exp(s_old - top_score[:, :, None])
    e_new = jnp.exp(s_new - top_score)
    denom_sum = jnp.sum(e_old, axis=2) + e_new
    p_old = (e_old / denom_sum[:, :, None]).astype(jnp.bfloat16)
    p_new = (e_new / denom_sum).astype(jnp.bfloat16)
    o_full = jnp.einsum("bhl,blc->bhc", p_old, cache_blk, preferred_element_type=jnp.float32) + p_new.astype(jnp.float32)[:, :, None] * kv_row.astype(jnp.float32)[:, None, :]
    o_lat = o_full[:, :, :latent].astype(jnp.bfloat16)
    v_head = jnp.einsum("bhc,hcv->bhv", o_lat, w_uv, preferred_element_type=jnp.float32).astype(jnp.bfloat16)
    attn_out = jnp.dot(v_head.reshape(num_seq, num_heads * v_dim), w_o, preferred_element_type=jnp.float32).astype(jnp.bfloat16)
    h_mid = (x_blk.astype(jnp.float32) + attn_out.astype(jnp.float32)).astype(jnp.bfloat16)
    return h_mid, kv_row


def chip_order(side):
    def hops(off):
        return sum(min(v, side - v) for v in off)

    offs = [(dx, dy) for dy in range(side) for dx in range(side)]
    return sorted(offs, key=lambda off: (hops(off), -max(min(v, side - v) for v in off), off))


def moe_kernel(n_dev, h_ref, oh_ref, gate_ref, shg_hbm, shu_hbm, shd_hbm, exg_hbm, exu_hbm, exd_hbm, out_ref,
               h_all, oh_all, rows, act, y_buf, back, wg, wu, wd, ring_g, ring_u, ring_d, sh_acc,
               ag_send, ag_recv, core_send, core_recv, oh_send_sem, oh_recv_sem, ret_send, ret_recv, w_sem, ring_sem, local_sem):
    side = int((n_dev // 2) ** 0.5)
    offs = chip_order(side)
    slot_of = {off: k for k, off in enumerate(offs)}
    n_chips = len(offs)
    me = lax.axis_index("ep")
    core = lax.rem(me, 2)
    my_x = lax.rem(me // 2, side)
    my_y = me // (2 * side)
    hidden = h_ref.shape[1]
    q4 = hidden // 4

    def device_at(off, c):
        return (lax.rem(my_y + off[1], side) * side + lax.rem(my_x + off[0], side)) * 2 + c

    def minus(a, b):
        return ((a[0] - b[0]) % side, (a[1] - b[1]) % side)

    partner = device_at((0, 0), 1 - core)

    n_exp = wg.shape[0]
    w_copies = []
    for e in range(n_exp):
        for m, (src, dst) in enumerate(((exg_hbm, wg), (exu_hbm, wu), (exd_hbm, wd))):
            cp = pltpu.make_async_copy(src.at[e], dst.at[e], w_sem.at[e * 3 + m])
            cp.start()
            w_copies.append(cp)
    n_ring, _, blk = ring_g.shape
    n_steps = shg_hbm.shape[1] // blk

    def ring_copies(step, slot):
        cols = pl.ds(pl.multiple_of(step * blk, blk), blk)
        return (pltpu.make_async_copy(shg_hbm.at[:, cols], ring_g.at[slot], ring_sem.at[0, slot]),
                pltpu.make_async_copy(shu_hbm.at[:, cols], ring_u.at[slot], ring_sem.at[1, slot]),
                pltpu.make_async_copy(shd_hbm.at[cols, :], ring_d.at[slot], ring_sem.at[2, slot]))

    for s in range(n_ring):
        for cp in ring_copies(s, s):
            cp.start()

    h_all[core] = h_ref[...]
    oh_all[core] = oh_ref[0, core]

    barrier = pltpu.get_barrier_semaphore()
    for i in range(1, n_dev):
        pl.semaphore_signal(barrier, inc=1, device_id={"ep": lax.rem(me + i, n_dev)}, device_id_type=MESH)
    pl.semaphore_wait(barrier, n_dev - 1)

    A, B = (0, 2), (2, 2)
    A1, A0, B0, B1 = (0, 1), (1, 1), (2, 1), (3, 1)
    xp, xm, yp, ym = (1, 0), (side - 1, 0), (0, 1), (0, side - 1)
    pieces, sends, core_pieces = {}, [], {}

    def cols_of(part):
        return pl.ds(part[0] * q4, part[1] * q4)

    def forward(off, part, d):
        dst_off = minus(off, d)
        n = len(pieces)
        src = h_ref if off == (0, 0) else h_all.at[slot_of[off] * 2 + core]
        cp = pltpu.make_async_remote_copy(
            src_ref=src.at[:, cols_of(part)], dst_ref=h_all.at[slot_of[dst_off] * 2 + core, :, cols_of(part)],
            send_sem=ag_send.at[n], recv_sem=ag_recv.at[n], device_id={"ep": device_at(d, core)}, device_id_type=MESH)
        cp.start()
        pieces[(dst_off, part)] = cp
        sends.append(cp)

    def to_partner(off, part):
        n = len(core_pieces)
        src = h_ref if off == (0, 0) else h_all.at[slot_of[off] * 2 + core]
        cp = pltpu.make_async_remote_copy(
            src_ref=src.at[:, cols_of(part)], dst_ref=h_all.at[slot_of[off] * 2 + core, :, cols_of(part)],
            send_sem=core_send.at[n], recv_sem=core_recv.at[n], device_id={"ep": partner}, device_id_type=MESH)
        cp.start()
        core_pieces[(off, part)] = cp
        sends.append(cp)

    def arrived(off, *parts):
        for part in parts:
            pieces[(off, part)].wait_recv()

    for d in (xp, xm):
        forward((0, 0), A, d)
    for d in (yp, ym):
        forward((0, 0), B, d)
    for d in (xp, xm):
        forward((0, 0), B, d)
    for d in (yp, ym):
        forward((0, 0), A, d)
    to_partner((0, 0), A)
    to_partner((0, 0), B)

    oh_copies = []
    for k, off in enumerate(offs):
        there = slot_of[minus((0, 0), off)]
        for c in ((None,) if k == 0 else (0, 1)):
            dst_core = 1 - core if c is None else c
            n = len(oh_copies)
            cp = pltpu.make_async_remote_copy(
                src_ref=oh_ref.at[there % 2, k * 2 + dst_core], dst_ref=oh_all.at[there * 2 + core],
                send_sem=oh_send_sem.at[n], recv_sem=oh_recv_sem.at[there * 2 + core],
                device_id={"ep": device_at(off, dst_core)}, device_id_type=MESH)
            cp.start()
            oh_copies.append(cp)
            sends.append(cp)

    for off, d, quarter in ((xm, xp, A0), (xp, xm, A1)):
        arrived(off, A)
        forward(off, A, yp)
        forward(off, A, ym)
        forward(off, quarter, d)
        to_partner(off, A)
    for off, d, quarter in ((ym, yp, B0), (yp, ym, B1)):
        arrived(off, B)
        forward(off, B, xp)
        forward(off, B, xm)
        forward(off, quarter, d)
        to_partner(off, B)
    for off, d, quarter in ((xm, xp, B0), (xp, xm, B1)):
        arrived(off, B)
        forward(off, quarter, d)
        to_partner(off, B)
    for off, d, quarter in ((ym, yp, A0), (yp, ym, A1)):
        arrived(off, A)
        forward(off, quarter, d)
        to_partner(off, A)
    x2, y2 = (2, 0), (0, 2)
    arrived(x2, A0, A1)
    forward(x2, A, yp)
    forward(x2, A, ym)
    to_partner(x2, A)
    arrived(y2, B0, B1)
    forward(y2, B, xp)
    forward(y2, B, xm)
    to_partner(y2, B)
    diagonals = [(dx, dy) for dy in (1, side - 1) for dx in (1, side - 1)]
    for off in diagonals:
        arrived(off, A)
        if off[1] == 1:
            forward(off, A1, ym)
        else:
            forward(off, A0, yp)
        to_partner(off, A)
        arrived(off, B)
        if off[0] == 1:
            forward(off, B1, xm)
        else:
            forward(off, B0, xp)
        to_partner(off, B)
    arrived(x2, B0, B1)
    to_partner(x2, B)
    arrived(y2, A0, A1)
    to_partner(y2, A)

    def hop3():
        for off, d, quarter in (((2, side - 1), yp, A0), ((2, 1), ym, A1)):
            arrived(off, A)
            forward(off, quarter, d)
            to_partner(off, A)
        for off, d, quarter in (((side - 1, 2), xp, B0), ((1, 2), xm, B1)):
            arrived(off, B)
            forward(off, quarter, d)
            to_partner(off, B)
        for off in ((2, side - 1), (2, 1)):
            arrived(off, B0, B1)
            to_partner(off, B)
        for off in ((side - 1, 2), (1, 2)):
            arrived(off, A0, A1)
            to_partner(off, A)

    def hop4():
        far = (2, 2)
        arrived(far, A0, A1)
        to_partner(far, A)
        arrived(far, B0, B1)
        to_partner(far, B)

    def ready(ks):
        for k in ks:
            for part in (A, B):
                core_pieces[(offs[k], part)].wait_recv()
            for c in ((1 - core,) if k == 0 else (0, 1)):
                pltpu.make_async_remote_copy(
                    src_ref=oh_ref.at[0, 0], dst_ref=oh_all.at[k * 2 + c], send_sem=oh_send_sem.at[0],
                    recv_sem=oh_recv_sem.at[k * 2 + c], device_id={"ep": partner}, device_id_type=MESH).wait_recv()

    half = n_chips // 2
    n_src = half * 2
    n_row = n_src * SLOTS_EXP
    seqs = h_ref.shape[0]
    ff = wg.shape[2]

    def gather_rows(k0):
        def body(g, carry):
            s0 = k0 * 2 + g * 4
            table = oh_all[pl.ds(s0, 4)].reshape(4 * 2 * SLOTS_EXP, LANES)
            toks = h_all.at[pl.ds(s0, 4)]
            for j in range(hidden // 512):
                got = jnp.dot(table, toks[:, :, j * 512:(j + 1) * 512].reshape(4 * seqs, 512), preferred_element_type=jnp.float32)
                got = got.reshape(4, n_exp, SLOTS_EXP, 512)
                for e in range(n_exp):
                    rows[e, pl.ds(pl.multiple_of(g * 4 * SLOTS_EXP, 4 * SLOTS_EXP), 4 * SLOTS_EXP), j * 512:(j + 1) * 512] = (
                        got[:, e].reshape(4 * SLOTS_EXP, 512).astype(jnp.bfloat16))
            return carry

        lax.fori_loop(0, half // 2, body, 0)

    def gate_up(e):
        r = rows.at[e]
        full = ff // 256
        for j in range(full):
            cs = slice(j * 256, (j + 1) * 256)
            g = jnp.dot(r[...], wg[e, :, cs], preferred_element_type=jnp.float32)
            u = jnp.dot(r[...], wu[e, :, cs], preferred_element_type=jnp.float32)
            act[e, :, cs] = (jax.nn.silu(g) * u).astype(jnp.bfloat16)
        if ff % 256:
            cs = slice(full * 256, ff)
            wid = ff - full * 256
            both = jnp.dot(r[...], jnp.concatenate([wg[e, :, cs], wu[e, :, cs]], axis=1), preferred_element_type=jnp.float32)
            act[e, :, cs] = (jax.nn.silu(both[:, :wid]) * both[:, wid:]).astype(jnp.bfloat16)

    def down(k0):
        for j in range(hidden // 256):
            cs = slice(j * 256, (j + 1) * 256)
            outs = [jnp.dot(act[e], wd[e, :, cs], preferred_element_type=jnp.float32).reshape(n_src, 1, SLOTS_EXP, 256) for e in range(n_exp)]
            y_buf[k0 * 2:k0 * 2 + n_src, :, cs] = jnp.concatenate(outs, axis=1).reshape(n_src, n_exp * SLOTS_EXP, 256).astype(jnp.bfloat16)

    ret_count = [0]

    def give_back(ks):
        for k in ks:
            there = slot_of[minus((0, 0), offs[k])]
            for c in ((None,) if k == 0 else (0, 1)):
                dst_core = 1 - core if c is None else c
                cp = pltpu.make_async_remote_copy(
                    src_ref=y_buf.at[k * 2 + dst_core], dst_ref=back.at[there * 2 + core],
                    send_sem=ret_send.at[ret_count[0]], recv_sem=ret_recv.at[there * 2 + core],
                    device_id={"ep": device_at(offs[k], dst_core)}, device_id_type=MESH)
                cp.start()
                ret_count[0] += 1
                sends.append(cp)

    near, far = list(range(half)), list(range(half, n_chips))
    ready(near)
    gather_rows(0)
    for e in range(n_exp):
        w_copies[e * 3].wait()
        w_copies[e * 3 + 1].wait()
        gate_up(e)
        if e == 0:
            hop3()
    for e in range(n_exp):
        w_copies[e * 3 + 2].wait()
    hop4()
    down(0)
    own = pltpu.make_async_copy(y_buf.at[core], back.at[core], local_sem)
    own.start()
    give_back(near[::-1])

    ready(far)
    gather_rows(half)

    def far_gate_up(e, carry):
        gate_up(e)
        return carry

    lax.fori_loop(0, n_exp, far_gate_up, 0)
    down(half)
    give_back(far[::-1])

    sh_acc[...] = jnp.zeros_like(sh_acc)

    def shared_step(i, carry):
        slot = lax.rem(i, n_ring)
        for cp in ring_copies(i, slot):
            cp.wait()
        g = jnp.dot(h_ref[...], ring_g[slot], preferred_element_type=jnp.float32)
        u = jnp.dot(h_ref[...], ring_u[slot], preferred_element_type=jnp.float32)
        a = (jax.nn.silu(g) * u).astype(jnp.bfloat16)
        sh_acc[...] += jnp.dot(a, ring_d[slot], preferred_element_type=jnp.float32)

        @pl.when(i + n_ring < n_steps)
        def _():
            for cp in ring_copies(i + n_ring, slot):
                cp.start()

        return carry

    lax.fori_loop(0, n_steps, shared_step, 0)

    gates = gate_ref[...]
    g0 = gates.astype(jnp.bfloat16)
    rest = gates - g0.astype(jnp.float32)
    g1 = rest.astype(jnp.bfloat16)
    g2 = (rest - g1.astype(jnp.float32)).astype(jnp.bfloat16)
    gates3 = jnp.concatenate([g0, g1, g2], axis=0)
    own.wait()
    for k in range(n_chips):
        for c in ((1 - core,) if k == 0 else (0, 1)):
            pltpu.make_async_remote_copy(
                src_ref=y_buf.at[0], dst_ref=back.at[k * 2 + c], send_sem=ret_send.at[0],
                recv_sem=ret_recv.at[k * 2 + c], device_id={"ep": partner}, device_id_type=MESH).wait_recv()
    n_slot = n_chips * 2 * n_exp * SLOTS_EXP
    for j in range(hidden // 256):
        cs = slice(j * 256, (j + 1) * 256)
        part = jnp.dot(gates3, back[:, :, cs].reshape(n_slot, 256), preferred_element_type=jnp.float32)
        routed = part[:seqs] + part[seqs:2 * seqs] + part[2 * seqs:]
        shared = sh_acc[:, cs].astype(jnp.bfloat16).astype(jnp.float32)
        out_ref[:, cs] = (h_ref[:, cs].astype(jnp.float32) + shared + routed).astype(jnp.bfloat16)
    for cp in sends:
        cp.wait_send()


def slot_tables(routes, route_gates, n_dev, local_exp, top_slots):
    side = int((n_dev // 2) ** 0.5)
    offs = jnp.array(chip_order(side), jnp.int32)
    me = lax.axis_index("ep")
    core, my_x, my_y = me % 2, (me // 2) % side, me // (2 * side)
    chips = ((my_y + offs[:, 1]) % side) * side + (my_x + offs[:, 0]) % side
    devs = chips[:, None] * 2 + jnp.arange(2)[None, :]
    ids = devs[:, :, None] * local_exp + jnp.arange(local_exp)[None, None, :]
    ids = jnp.broadcast_to(ids[:, :, :, None], ids.shape + (top_slots,)).reshape(-1)
    pos = jnp.arange(ids.shape[0]) % top_slots
    seqs = routes.shape[0]
    hit = routes[None, :, :] == ids[:, None, None]
    has = jnp.any(hit, axis=2)
    earlier = jnp.arange(seqs)[:, None] < jnp.arange(seqs)[None, :]
    rank = jnp.dot(has.astype(jnp.bfloat16), earlier.astype(jnp.bfloat16), preferred_element_type=jnp.float32)
    sel = has & (rank == pos[:, None].astype(jnp.float32))
    gate = jnp.sum(jnp.where(hit & sel[:, :, None], route_gates[None, :, :], 0.0), axis=2).T
    wide = jnp.tile(sel, (1, LANES // seqs))
    lane_blk = jnp.arange(LANES) // seqs
    table = jnp.stack([wide & (lane_blk == 2 * v + core)[None, :] for v in range(2)]).astype(jnp.bfloat16)
    return table.reshape(2, n_dev, local_exp * top_slots, LANES), gate


def moe_call(n_dev, h_mid, table, gate, sh_gate, sh_up, sh_down, ex_gate, ex_up, ex_down):
    seqs, hidden = h_mid.shape
    n_exp, _, ff = ex_gate.shape
    n_chips = n_dev // 2
    n_src = n_chips
    slots = n_exp * SLOTS_EXP
    n_ring, blk = 4, 256
    bf = jnp.bfloat16
    dma = pltpu.SemaphoreType.DMA
    vmem = pl.BlockSpec(memory_space=pltpu.VMEM)
    hbm = pl.BlockSpec(memory_space=pl.ANY)
    return pl.pallas_call(
        functools.partial(moe_kernel, n_dev),
        out_shape=jax.ShapeDtypeStruct((seqs, hidden), bf),
        in_specs=[vmem] * 3 + [hbm] * 6,
        out_specs=vmem,
        scratch_shapes=[
            pltpu.VMEM((n_dev, seqs, hidden), bf),
            pltpu.VMEM((n_dev, slots, LANES), bf),
            pltpu.VMEM((n_exp, n_src * SLOTS_EXP, hidden), bf),
            pltpu.VMEM((n_exp, n_src * SLOTS_EXP, ff), bf),
            pltpu.VMEM((n_dev, slots, hidden), bf),
            pltpu.VMEM((n_dev, slots, hidden), bf),
            pltpu.VMEM((n_exp, hidden, ff), bf),
            pltpu.VMEM((n_exp, hidden, ff), bf),
            pltpu.VMEM((n_exp, ff, hidden), bf),
            pltpu.VMEM((n_ring, hidden, blk), bf),
            pltpu.VMEM((n_ring, hidden, blk), bf),
            pltpu.VMEM((n_ring, blk, hidden), bf),
            pltpu.VMEM((seqs, hidden), jnp.float32),
            dma((64,)), dma((64,)), dma((2 * n_chips,)), dma((2 * n_chips,)),
            dma((n_dev,)), dma((n_dev,)), dma((n_dev,)), dma((n_dev,)),
            dma((n_exp * 3,)), dma((3, n_ring)), dma,
        ],
        compiler_params=pltpu.CompilerParams(collective_id=0, has_side_effects=True, vmem_limit_bytes=67043328),
    )(h_mid, table, gate, sh_gate, sh_up, sh_down, ex_gate, ex_up, ex_down)


def solution(mesh):
    group_size = mesh.shape["ep"]

    def device_step(x_blk, cache_blk, len_blk, routes, route_gates, w_q, w_dkv, w_uk, w_uv, w_o, sh_gate, sh_up, sh_down, ex_gate, ex_up, ex_down):
        h_mid, kv_row = attend_local(x_blk, cache_blk, len_blk, w_q, w_dkv, w_uk, w_uv, w_o)
        table, gate = slot_tables(routes, route_gates, group_size, ex_gate.shape[0], SLOTS_EXP)
        layer_out = moe_call(group_size, h_mid, table, gate, sh_gate, sh_up, sh_down, ex_gate, ex_up, ex_down)
        return layer_out, kv_row

    batch_spec = P(("dp", "ep"))
    weight_spec = P()
    expert_spec = P("ep")
    in_specs = (batch_spec,) * 5 + (weight_spec,) * 8 + (expert_spec,) * 3
    return jax.shard_map(device_step, mesh=mesh, in_specs=in_specs, out_specs=(batch_spec, batch_spec), check_vma=False)
```

```python
import functools

import jax
import jax.numpy as jnp
from jax import lax
from jax.experimental import pallas as pl
from jax.experimental.pallas import tpu as pltpu
from jax.sharding import PartitionSpec as P

MESH = pl.DeviceIdType.MESH
SLOTS_EXP = 8
LANES = 128

def attention(x_ref, lens_ref, cache_hbm, wq_hbm, wdkv_hbm, wuk_hbm, wuv_hbm, wo_hbm, kv_ref, h_out,
              wq, wdkv, wuk, wuv, wo, cache, q_rows, kv_rows, o_rows, v_rows, a_sem, c_sem, while_loading):
    seqs, hidden = x_ref.shape
    heads, nope, latent = wuk.shape
    rope = wdkv.shape[0] - latent
    v_dim = wuv.shape[2]
    pair = 2 * (nope + rope)
    n_q = 4
    q_blk = wq.shape[1] // n_q
    c_blk = seqs // c_sem.shape[0]
    copies = {}

    def fetch(name, src, dst):
        cp = pltpu.make_async_copy(src, dst, a_sem.at[len(copies)])
        cp.start()
        copies[name] = cp

    fetch("dkv", wdkv_hbm, wdkv)
    for i in range(n_q):
        fetch(i, wq_hbm.at[:, i * q_blk:(i + 1) * q_blk], wq.at[:, i * q_blk:(i + 1) * q_blk])
        if i == 0:
            fetch("uk", wuk_hbm, wuk)

    def cache_copy(i):
        rows_b = pl.ds(i * c_blk, c_blk)
        return pltpu.make_async_copy(cache_hbm.at[rows_b], cache.at[rows_b], c_sem.at[i])

    for i in range(seqs // c_blk):
        cache_copy(i).start()
    fetch("uv", wuv_hbm, wuv)
    fetch("o", wo_hbm, wo)

    while_loading()
    lane = lax.broadcasted_iota(jnp.int32, (seqs, rope), 1)
    freq = jnp.exp(lax.rem(lane, rope // 2).astype(jnp.float32) * (-2.0 * jnp.log(10000.0) / rope))
    row = lax.broadcasted_iota(jnp.int32, (seqs, rope), 0)
    pos = jnp.zeros((seqs, rope), jnp.int32)
    for b in range(seqs):
        pos = jnp.where(row == b, lens_ref[b], pos)
    angle = pos.astype(jnp.float32) * freq
    cos_t = jnp.cos(angle)
    sin_t = jnp.where(lane < rope // 2, -jnp.sin(angle), jnp.sin(angle))

    def rotate(u):
        swapped = jnp.concatenate([u[:, rope // 2:], u[:, :rope // 2]], axis=1)
        return u * cos_t + swapped * sin_t

    contract_last = (((1,), (1,)), ((), ()))
    x = x_ref[...]
    copies["dkv"].wait()
    raw = lax.dot_general(x, wdkv[...], contract_last, preferred_element_type=jnp.float32)
    lat = raw[:, :latent].astype(jnp.bfloat16)
    pe = rotate(raw[:, latent:latent + rope]).astype(jnp.bfloat16)
    kv_ref[:, :latent] = lat
    kv_ref[:, latent:latent + rope] = pe
    kv_rows[:, :latent] = lat.astype(jnp.float32)
    kv_rows[:, latent:latent + rope] = pe.astype(jnp.float32)

    n_lat = latent // LANES
    for p in range(heads // 2):
        if (p * pair) % q_blk == 0:
            copies[p * pair // q_blk].wait()
        if p == 0:
            copies["uk"].wait()
        qp = jnp.dot(x, wq[:, p * pair:(p + 1) * pair], preferred_element_type=jnp.float32).astype(jnp.bfloat16).astype(jnp.float32)
        for i in range(2):
            h = 2 * p + i
            base = i * (nope + rope)
            q_n = qp[:, base:base + nope].astype(jnp.bfloat16)
            q_lat = jnp.dot(q_n, wuk[h], preferred_element_type=jnp.float32)
            q_pe = rotate(qp[:, base + nope:base + nope + rope])
            q_lat = q_lat.astype(jnp.bfloat16).astype(jnp.float32)
            for t in range(n_lat):
                q_rows[t, h * seqs:(h + 1) * seqs, :] = q_lat[:, t * LANES:(t + 1) * LANES]
            q_rows[n_lat, h * seqs:(h + 1) * seqs, :rope] = q_pe.astype(jnp.bfloat16).astype(jnp.float32)

    scale = (nope + rope) ** -0.5
    keys = cache.shape[2]
    key_id = lax.broadcasted_iota(jnp.int32, (heads, keys), 1)

    def attend(i, carry):
        cache_copy(i).wait()
        ids = [i * c_blk + j for j in range(c_blk)]
        qs = [[q_rows[t, pl.ds(b, heads, stride=seqs), :] for t in range(n_lat + 1)] for b in ids]
        s_old, s_new, kls = [], [], []
        for b, q in zip(ids, qs):
            ql, qr = jnp.concatenate(q[:n_lat], axis=1), q[n_lat][:, :rope]
            s_old.append(jnp.dot(ql.astype(jnp.bfloat16), cache[b, :latent, :], preferred_element_type=jnp.float32)
                         + jnp.dot(qr.astype(jnp.bfloat16), cache[b, latent:latent + rope, :], preferred_element_type=jnp.float32))
        for b, q in zip(ids, qs):
            kv = kv_rows[pl.ds(b, 1), :]
            prod = q[0] * kv[:, :LANES]
            for t in range(1, n_lat):
                prod += q[t] * kv[:, t * LANES:(t + 1) * LANES]
            s_new.append(jnp.sum(prod, axis=1, keepdims=True)
                         + jnp.sum(q[n_lat][:, :rope] * kv[:, latent:latent + rope], axis=1, keepdims=True))
            kls.append(kv[:, :latent])
        s_old = [jnp.where(key_id < lens_ref[b], s * scale, -jnp.inf) for b, s in zip(ids, s_old)]
        s_old = jnp.concatenate(s_old, axis=0)
        s_new = jnp.concatenate(s_new, axis=0) * scale
        top = jnp.maximum(jnp.max(s_old, axis=1, keepdims=True), s_new)
        e_old = jnp.exp(s_old - top)
        e_new = jnp.exp(s_new - top)
        total = jnp.sum(e_old, axis=1, keepdims=True) + e_new
        p_old = (e_old / total).astype(jnp.bfloat16)
        p_new = (e_new / total).astype(jnp.bfloat16).astype(jnp.float32)
        for j, b in enumerate(ids):
            hs = slice(j * heads, (j + 1) * heads)
            o = lax.dot_general(p_old[hs], cache[b, :latent, :], contract_last, preferred_element_type=jnp.float32) + p_new[hs] * kls[j]
            for t in range(n_lat):
                o_rows[t, pl.ds(b, heads, stride=seqs), :] = o[:, t * LANES:(t + 1) * LANES]
        return carry

    lax.fori_loop(0, seqs // c_blk, attend, 0)

    copies["uv"].wait()
    for h in range(heads):
        o = jnp.concatenate([o_rows[t, h * seqs:(h + 1) * seqs, :] for t in range(n_lat)], axis=1).astype(jnp.bfloat16)
        v_rows[:, h * v_dim:(h + 1) * v_dim] = jnp.dot(o, wuv[h], preferred_element_type=jnp.float32).astype(jnp.bfloat16)
    copies["o"].wait()
    for j in range(hidden // 256):
        cs = slice(j * 256, (j + 1) * 256)
        a = jnp.dot(v_rows[...], wo[:, cs], preferred_element_type=jnp.float32).astype(jnp.bfloat16)
        h_out[:, cs] = (x_ref[:, cs].astype(jnp.float32) + a.astype(jnp.float32)).astype(jnp.bfloat16)


def attention_scratch(seqs, hidden, heads, nope, latent, rope, v_dim, keys):
    bf = jnp.bfloat16
    wide = latent + LANES
    return [pltpu.VMEM((hidden, heads * (nope + rope)), bf), pltpu.VMEM((latent + rope, hidden), bf),
            pltpu.VMEM((heads, nope, latent), bf), pltpu.VMEM((heads, latent, v_dim), bf),
            pltpu.VMEM((heads * v_dim, hidden), bf), pltpu.VMEM((seqs, latent + rope, keys), bf),
            pltpu.VMEM((wide // LANES, heads * seqs, LANES), jnp.float32), pltpu.VMEM((seqs, wide), jnp.float32),
            pltpu.VMEM((latent // LANES, heads * seqs, LANES), jnp.float32), pltpu.VMEM((seqs, heads * v_dim), bf),
            pltpu.SemaphoreType.DMA((8,)), pltpu.SemaphoreType.DMA((4,))]


def chip_order(side):
    def hops(off):
        return sum(min(v, side - v) for v in off)

    offs = [(dx, dy) for dy in range(side) for dx in range(side)]
    return sorted(offs, key=lambda off: (hops(off), -max(min(v, side - v) for v in off), off))


def layer_kernel(n_dev, x_ref, lens_ref, routes_ref, gates_ref, cache_hbm, wq_hbm, wdkv_hbm, wuk_hbm, wuv_hbm, wo_hbm,
                 shg_hbm, shu_hbm, shd_hbm, exg_hbm, exu_hbm, exd_hbm, out_ref, kv_ref,
                 h_ref, oh_ref, gate_ref, h_all, oh_all, rows, act, y_buf, back, sh_acc,
                 ag_send, ag_recv, core_send, core_recv, oh_send_sem, oh_recv_sem, ret_send, ret_recv, local_sem):
    barrier = pltpu.get_barrier_semaphore()
    me = lax.axis_index("ep")
    for i in range(1, n_dev):
        pl.semaphore_signal(barrier, inc=1, device_id={"ep": lax.rem(me + i, n_dev)}, device_id_type=MESH)

    seqs, hidden = x_ref.shape
    heads, nope, latent = wuk_hbm.shape

    def attend(*scratch):
        attention(x_ref, lens_ref, cache_hbm, wq_hbm, wdkv_hbm, wuk_hbm, wuv_hbm, wo_hbm, kv_ref, h_ref, *scratch,
                  while_loading=lambda: slot_tables(n_dev, routes_ref, gates_ref, oh_ref, gate_ref))

    pl.run_scoped(attend, *attention_scratch(seqs, hidden, heads, nope, latent, wdkv_hbm.shape[0] - latent, wuv_hbm.shape[2], cache_hbm.shape[2]))

    def experts(*scratch):
        moe(n_dev, h_ref, oh_ref, gate_ref, shg_hbm, shu_hbm, shd_hbm, exg_hbm, exu_hbm, exd_hbm, out_ref,
            h_all, oh_all, rows, act, y_buf, back, *scratch[:-2], sh_acc,
            ag_send, ag_recv, core_send, core_recv, oh_send_sem, oh_recv_sem, ret_send, ret_recv, *scratch[-2:], local_sem)

    n_exp, _, ff = exg_hbm.shape
    n_ring, blk = 4, 256
    bf = jnp.bfloat16
    pl.run_scoped(
        experts,
        pltpu.VMEM((n_exp, hidden, ff), bf), pltpu.VMEM((n_exp, hidden, ff), bf), pltpu.VMEM((n_exp, ff, hidden), bf),
        pltpu.VMEM((n_ring, hidden, blk), bf), pltpu.VMEM((n_ring, hidden, blk), bf), pltpu.VMEM((n_ring, blk, hidden), bf),
        pltpu.SemaphoreType.DMA((n_exp * 3,)), pltpu.SemaphoreType.DMA((3, n_ring)))


def moe(n_dev, h_ref, oh_ref, gate_ref, shg_hbm, shu_hbm, shd_hbm, exg_hbm, exu_hbm, exd_hbm, out_ref,
        h_all, oh_all, rows, act, y_buf, back, wg, wu, wd, ring_g, ring_u, ring_d, sh_acc,
        ag_send, ag_recv, core_send, core_recv, oh_send_sem, oh_recv_sem, ret_send, ret_recv, w_sem, ring_sem, local_sem):
    side = int((n_dev // 2) ** 0.5)
    offs = chip_order(side)
    slot_of = {off: k for k, off in enumerate(offs)}
    n_chips = len(offs)
    me = lax.axis_index("ep")
    core = lax.rem(me, 2)
    my_x = lax.rem(me // 2, side)
    my_y = me // (2 * side)
    hidden = h_ref.shape[1]
    q4 = hidden // 4

    def device_at(off, c):
        return (lax.rem(my_y + off[1], side) * side + lax.rem(my_x + off[0], side)) * 2 + c

    def minus(a, b):
        return ((a[0] - b[0]) % side, (a[1] - b[1]) % side)

    partner = device_at((0, 0), 1 - core)

    n_exp = wg.shape[0]
    w_copies = []
    for e in range(n_exp):
        for m, (src, dst) in enumerate(((exg_hbm, wg), (exu_hbm, wu), (exd_hbm, wd))):
            cp = pltpu.make_async_copy(src.at[e], dst.at[e], w_sem.at[e * 3 + m])
            cp.start()
            w_copies.append(cp)
    n_ring, _, blk = ring_g.shape
    n_steps = shg_hbm.shape[1] // blk

    def ring_copies(step, slot):
        cols = pl.ds(pl.multiple_of(step * blk, blk), blk)
        return (pltpu.make_async_copy(shg_hbm.at[:, cols], ring_g.at[slot], ring_sem.at[0, slot]),
                pltpu.make_async_copy(shu_hbm.at[:, cols], ring_u.at[slot], ring_sem.at[1, slot]),
                pltpu.make_async_copy(shd_hbm.at[cols, :], ring_d.at[slot], ring_sem.at[2, slot]))

    for s in range(n_ring):
        for cp in ring_copies(s, s):
            cp.start()

    h_all[core] = h_ref[...]
    oh_all[core] = oh_ref[0, core]

    pl.semaphore_wait(pltpu.get_barrier_semaphore(), n_dev - 1)

    A, B = (0, 2), (2, 2)
    A1, A0, B0, B1 = (0, 1), (1, 1), (2, 1), (3, 1)
    xp, xm, yp, ym = (1, 0), (side - 1, 0), (0, 1), (0, side - 1)
    pieces, sends, core_pieces = {}, [], {}

    def cols_of(part):
        return pl.ds(part[0] * q4, part[1] * q4)

    def forward(off, part, d):
        dst_off = minus(off, d)
        n = len(pieces)
        src = h_ref if off == (0, 0) else h_all.at[slot_of[off] * 2 + core]
        cp = pltpu.make_async_remote_copy(
            src_ref=src.at[:, cols_of(part)], dst_ref=h_all.at[slot_of[dst_off] * 2 + core, :, cols_of(part)],
            send_sem=ag_send.at[n], recv_sem=ag_recv.at[n], device_id={"ep": device_at(d, core)}, device_id_type=MESH)
        cp.start()
        pieces[(dst_off, part)] = cp
        sends.append(cp)

    def to_partner(off, part):
        n = len(core_pieces)
        src = h_ref if off == (0, 0) else h_all.at[slot_of[off] * 2 + core]
        cp = pltpu.make_async_remote_copy(
            src_ref=src.at[:, cols_of(part)], dst_ref=h_all.at[slot_of[off] * 2 + core, :, cols_of(part)],
            send_sem=core_send.at[n], recv_sem=core_recv.at[n], device_id={"ep": partner}, device_id_type=MESH)
        cp.start()
        core_pieces[(off, part)] = cp
        sends.append(cp)

    def arrived(off, *parts):
        for part in parts:
            pieces[(off, part)].wait_recv()

    for d in (xp, xm):
        forward((0, 0), A, d)
    for d in (yp, ym):
        forward((0, 0), B, d)
    for d in (xp, xm):
        forward((0, 0), B, d)
    for d in (yp, ym):
        forward((0, 0), A, d)
    to_partner((0, 0), A)
    to_partner((0, 0), B)

    oh_copies = []
    for k, off in enumerate(offs):
        there = slot_of[minus((0, 0), off)]
        for c in ((None,) if k == 0 else (0, 1)):
            dst_core = 1 - core if c is None else c
            n = len(oh_copies)
            cp = pltpu.make_async_remote_copy(
                src_ref=oh_ref.at[there % 2, k * 2 + dst_core], dst_ref=oh_all.at[there * 2 + core],
                send_sem=oh_send_sem.at[n], recv_sem=oh_recv_sem.at[there * 2 + core],
                device_id={"ep": device_at(off, dst_core)}, device_id_type=MESH)
            cp.start()
            oh_copies.append(cp)
            sends.append(cp)

    for off, d, quarter in ((xm, xp, A0), (xp, xm, A1)):
        arrived(off, A)
        forward(off, A, yp)
        forward(off, A, ym)
        forward(off, quarter, d)
        to_partner(off, A)
    for off, d, quarter in ((ym, yp, B0), (yp, ym, B1)):
        arrived(off, B)
        forward(off, B, xp)
        forward(off, B, xm)
        forward(off, quarter, d)
        to_partner(off, B)
    for off, d, quarter in ((xm, xp, B0), (xp, xm, B1)):
        arrived(off, B)
        forward(off, quarter, d)
        to_partner(off, B)
    for off, d, quarter in ((ym, yp, A0), (yp, ym, A1)):
        arrived(off, A)
        forward(off, quarter, d)
        to_partner(off, A)
    x2, y2 = (2, 0), (0, 2)
    arrived(x2, A0, A1)
    forward(x2, A, yp)
    forward(x2, A, ym)
    to_partner(x2, A)
    arrived(y2, B0, B1)
    forward(y2, B, xp)
    forward(y2, B, xm)
    to_partner(y2, B)
    diagonals = [(dx, dy) for dy in (1, side - 1) for dx in (1, side - 1)]
    for off in diagonals:
        arrived(off, A)
        if off[1] == 1:
            forward(off, A1, ym)
        else:
            forward(off, A0, yp)
        to_partner(off, A)
        arrived(off, B)
        if off[0] == 1:
            forward(off, B1, xm)
        else:
            forward(off, B0, xp)
        to_partner(off, B)
    arrived(x2, B0, B1)
    to_partner(x2, B)
    arrived(y2, A0, A1)
    to_partner(y2, A)

    def hop3():
        for off, d, quarter in (((2, side - 1), yp, A0), ((2, 1), ym, A1)):
            arrived(off, A)
            forward(off, quarter, d)
            to_partner(off, A)
        for off, d, quarter in (((side - 1, 2), xp, B0), ((1, 2), xm, B1)):
            arrived(off, B)
            forward(off, quarter, d)
            to_partner(off, B)
        for off in ((2, side - 1), (2, 1)):
            arrived(off, B0, B1)
            to_partner(off, B)
        for off in ((side - 1, 2), (1, 2)):
            arrived(off, A0, A1)
            to_partner(off, A)

    def hop4():
        far = (2, 2)
        arrived(far, A0, A1)
        to_partner(far, A)
        arrived(far, B0, B1)
        to_partner(far, B)

    def ready(ks):
        for k in ks:
            for part in (A, B):
                core_pieces[(offs[k], part)].wait_recv()
            for c in ((1 - core,) if k == 0 else (0, 1)):
                pltpu.make_async_remote_copy(
                    src_ref=oh_ref.at[0, 0], dst_ref=oh_all.at[k * 2 + c], send_sem=oh_send_sem.at[0],
                    recv_sem=oh_recv_sem.at[k * 2 + c], device_id={"ep": partner}, device_id_type=MESH).wait_recv()

    half = n_chips // 2
    n_src = half * 2
    n_row = n_src * SLOTS_EXP
    seqs = h_ref.shape[0]
    ff = wg.shape[2]

    def gather_rows(k0):
        for g in range(half // 2):
            s0 = k0 * 2 + g * 4
            table = oh_all[s0:s0 + 4].reshape(4 * 2 * SLOTS_EXP, LANES)
            got = jnp.dot(table, h_all[s0:s0 + 4].reshape(4 * seqs, hidden), preferred_element_type=jnp.float32)
            got = got.reshape(4, n_exp, SLOTS_EXP, hidden)
            for e in range(n_exp):
                rows[e, g * 4 * SLOTS_EXP:(g + 1) * 4 * SLOTS_EXP, :] = got[:, e].reshape(4 * SLOTS_EXP, hidden).astype(jnp.bfloat16)

    def gate_up(e):
        r = rows.at[e]
        full = ff // 256
        for j in range(full):
            cs = slice(j * 256, (j + 1) * 256)
            g = jnp.dot(r[...], wg[e, :, cs], preferred_element_type=jnp.float32)
            u = jnp.dot(r[...], wu[e, :, cs], preferred_element_type=jnp.float32)
            act[e, :, cs] = (jax.nn.silu(g) * u).astype(jnp.bfloat16)
        if ff % 256:
            cs = slice(full * 256, ff)
            wid = ff - full * 256
            both = jnp.dot(r[...], jnp.concatenate([wg[e, :, cs], wu[e, :, cs]], axis=1), preferred_element_type=jnp.float32)
            act[e, :, cs] = (jax.nn.silu(both[:, :wid]) * both[:, wid:]).astype(jnp.bfloat16)

    def down(k0):
        for j in range(hidden // 256):
            cs = slice(j * 256, (j + 1) * 256)
            outs = [jnp.dot(act[e], wd[e, :, cs], preferred_element_type=jnp.float32).reshape(n_src, 1, SLOTS_EXP, 256) for e in range(n_exp)]
            y_buf[k0 * 2:k0 * 2 + n_src, :, cs] = jnp.concatenate(outs, axis=1).reshape(n_src, n_exp * SLOTS_EXP, 256).astype(jnp.bfloat16)

    ret_count = [0]

    def give_back(ks):
        for k in ks:
            there = slot_of[minus((0, 0), offs[k])]
            for c in ((None,) if k == 0 else (0, 1)):
                dst_core = 1 - core if c is None else c
                cp = pltpu.make_async_remote_copy(
                    src_ref=y_buf.at[k * 2 + dst_core], dst_ref=back.at[there * 2 + core],
                    send_sem=ret_send.at[ret_count[0]], recv_sem=ret_recv.at[there * 2 + core],
                    device_id={"ep": device_at(offs[k], dst_core)}, device_id_type=MESH)
                cp.start()
                ret_count[0] += 1
                sends.append(cp)

    near, far = list(range(half)), list(range(half, n_chips))
    ready(near)
    gather_rows(0)
    for e in range(n_exp):
        w_copies[e * 3].wait()
        w_copies[e * 3 + 1].wait()
        gate_up(e)
        if e == 0:
            hop3()
    for e in range(n_exp):
        w_copies[e * 3 + 2].wait()
    hop4()
    down(0)
    own = pltpu.make_async_copy(y_buf.at[core], back.at[core], local_sem)
    own.start()
    give_back(near[::-1])

    ready(far)
    gather_rows(half)

    def far_gate_up(e, carry):
        gate_up(e)
        return carry

    lax.fori_loop(0, n_exp, far_gate_up, 0)
    down(half)
    give_back(far[::-1])

    sh_acc[...] = jnp.zeros_like(sh_acc)

    def shared_step(i, carry):
        slot = lax.rem(i, n_ring)
        for cp in ring_copies(i, slot):
            cp.wait()
        g = jnp.dot(h_ref[...], ring_g[slot], preferred_element_type=jnp.float32)
        u = jnp.dot(h_ref[...], ring_u[slot], preferred_element_type=jnp.float32)
        a = (jax.nn.silu(g) * u).astype(jnp.bfloat16)
        sh_acc[...] += jnp.dot(a, ring_d[slot], preferred_element_type=jnp.float32)

        @pl.when(i + n_ring < n_steps)
        def _():
            for cp in ring_copies(i + n_ring, slot):
                cp.start()

        return carry

    lax.fori_loop(0, n_steps, shared_step, 0)

    own.wait()
    for k in range(n_chips):
        for c in ((1 - core,) if k == 0 else (0, 1)):
            pltpu.make_async_remote_copy(
                src_ref=y_buf.at[0], dst_ref=back.at[k * 2 + c], send_sem=ret_send.at[0],
                recv_sem=ret_recv.at[k * 2 + c], device_id={"ep": partner}, device_id_type=MESH).wait_recv()
    n_slot = n_chips * 2 * n_exp * SLOTS_EXP
    for j in range(hidden // 256):
        cs = slice(j * 256, (j + 1) * 256)
        part = lax.dot_general(gate_ref[...], back[:, :, cs].reshape(n_slot, 256), (((0,), (0,)), ((), ())), preferred_element_type=jnp.float32)
        routed = part[:seqs] + part[seqs:2 * seqs] + part[2 * seqs:3 * seqs]
        shared = sh_acc[:, cs].astype(jnp.bfloat16).astype(jnp.float32)
        out_ref[:, cs] = (h_ref[:, cs].astype(jnp.float32) + shared + routed).astype(jnp.bfloat16)
    for cp in sends:
        cp.wait_send()


def slot_tables(n_dev, routes_ref, gates_ref, oh_ref, gate_ref):
    side = int((n_dev // 2) ** 0.5)
    me = lax.axis_index("ep")
    core, my_x, my_y = lax.rem(me, 2), lax.rem(me // 2, side), me // (2 * side)
    top_k, seqs = routes_ref.shape
    per_chip = oh_ref.shape[1] * oh_ref.shape[2] // (n_dev // 2)
    row = lax.broadcasted_iota(jnp.int32, (per_chip, LANES), 0)
    exp_chip = per_chip // SLOTS_EXP
    ids = jnp.concatenate([
        row // SLOTS_EXP + exp_chip * (lax.rem(my_y + dy, side) * side + lax.rem(my_x + dx, side))
        for dx, dy in chip_order(side)], axis=0)
    n_slot = ids.shape[0]
    pos = lax.rem(lax.broadcasted_iota(jnp.int32, (n_slot, LANES), 0), SLOTS_EXP)
    block = lax.broadcasted_iota(jnp.int32, (n_slot, LANES), 1) // seqs
    routes = jnp.concatenate([routes_ref[...]] * (LANES // seqs), axis=1)
    gates = jnp.concatenate([gates_ref[...]] * (LANES // seqs), axis=1)
    has = jnp.zeros((n_slot, LANES), jnp.float32)
    gate = jnp.zeros((n_slot, LANES), jnp.float32)
    for k in range(top_k):
        hit = ids == routes[k:k + 1, :]
        has = jnp.where(hit, 1.0, has)
        gate = jnp.where(hit, gates[k:k + 1, :], gate)
    src = lax.broadcasted_iota(jnp.int32, (LANES, LANES), 0)
    dst = lax.broadcasted_iota(jnp.int32, (LANES, LANES), 1)
    earlier = jnp.where((src < dst) & (src // seqs == dst // seqs), 1.0, 0.0).astype(jnp.bfloat16)
    rank = jnp.dot(has.astype(jnp.bfloat16), earlier, preferred_element_type=jnp.float32)
    sel = jnp.where(rank == pos.astype(jnp.float32), has, 0.0)
    for v in range(2):
        oh_ref[v] = jnp.where(block == 2 * v + core, sel, 0.0).astype(jnp.bfloat16).reshape(oh_ref.shape[1:])
    gate = gate * sel
    g0 = gate.astype(jnp.bfloat16).astype(jnp.float32)
    g1 = (gate - g0).astype(jnp.bfloat16).astype(jnp.float32)
    g2 = gate - g0 - g1
    gate_ref[...] = jnp.where(block == 0, g0, jnp.where(block == 1, g1, jnp.where(block == 2, g2, 0.0))).astype(jnp.bfloat16)


def solution(mesh):
    n_dev = mesh.shape["ep"]

    def device_step(x_blk, cache_blk, len_blk, routes, route_gates, w_q, w_dkv, w_uk, w_uv, w_o, sh_gate, sh_up, sh_down, ex_gate, ex_up, ex_down):
        seqs, hidden = x_blk.shape
        n_exp, _, ff = ex_gate.shape
        n_chips = n_dev // 2
        slots = n_exp * SLOTS_EXP
        half_rows = n_chips * SLOTS_EXP
        bf = jnp.bfloat16
        dma = pltpu.SemaphoreType.DMA
        vmem = pl.BlockSpec(memory_space=pltpu.VMEM)
        hbm = pl.BlockSpec(memory_space=pl.ANY)
        layer_out, kv_row = pl.pallas_call(
            functools.partial(layer_kernel, n_dev),
            out_shape=(jax.ShapeDtypeStruct((seqs, hidden), bf), jax.ShapeDtypeStruct((seqs, w_dkv.shape[1]), bf)),
            in_specs=[vmem, pl.BlockSpec(memory_space=pltpu.SMEM), vmem, vmem] + [hbm] * 12,
            out_specs=(vmem, vmem),
            scratch_shapes=[
                pltpu.VMEM((seqs, hidden), bf),
                pltpu.VMEM((2, n_dev, slots, LANES), bf),
                pltpu.VMEM((n_dev * slots, LANES), bf),
                pltpu.VMEM((n_dev, seqs, hidden), bf),
                pltpu.VMEM((n_dev, slots, LANES), bf),
                pltpu.VMEM((n_exp, half_rows, hidden), bf),
                pltpu.VMEM((n_exp, half_rows, ff), bf),
                pltpu.VMEM((n_dev, slots, hidden), bf),
                pltpu.VMEM((n_dev, slots, hidden), bf),
                pltpu.VMEM((seqs, hidden), jnp.float32),
                dma((64,)), dma((64,)), dma((2 * n_chips,)), dma((2 * n_chips,)),
                dma((n_dev,)), dma((n_dev,)), dma((n_dev,)), dma((n_dev,)), dma,
            ],
            compiler_params=pltpu.CompilerParams(collective_id=0, has_side_effects=True, vmem_limit_bytes=67043328),
        )(x_blk, len_blk, routes.T, route_gates.T, cache_blk.transpose(0, 2, 1), w_q, w_dkv.T, w_uk, w_uv, w_o,
          sh_gate, sh_up, sh_down, ex_gate, ex_up, ex_down)
        return layer_out, kv_row

    batch_spec = P(("dp", "ep"))
    weight_spec = P()
    expert_spec = P("ep")
    in_specs = (batch_spec,) * 5 + (weight_spec,) * 8 + (expert_spec,) * 3
    return jax.shard_map(device_step, mesh=mesh, in_specs=in_specs, out_specs=(batch_spec, batch_spec), check_vma=False)
```

```python
import functools

import jax
import jax.numpy as jnp
from jax import lax
from jax.experimental import pallas as pl
from jax.experimental.pallas import tpu as pltpu
from jax.sharding import PartitionSpec as P

MESH = pl.DeviceIdType.MESH
SLOTS_EXP = 8
LANES = 128

def attention(x_ref, lens_ref, cache_hbm, wq_hbm, wdkv_hbm, wuk_hbm, wuv_hbm, wo_hbm, kv_ref, h_out,
              wq, wdkv, wuk, wuv, wo, cache, q_rows, kv_rows, o_rows, v_rows, a_sem, c_sem, while_loading):
    seqs, hidden = x_ref.shape
    heads, nope, latent = wuk.shape
    rope = wdkv.shape[0] - latent
    v_dim = wuv.shape[2]
    pair = 2 * (nope + rope)
    n_q = 4
    q_blk = wq.shape[1] // n_q
    c_blk = seqs // c_sem.shape[0]
    copies = {}

    def fetch(name, src, dst):
        cp = pltpu.make_async_copy(src, dst, a_sem.at[len(copies)])
        cp.start()
        copies[name] = cp

    fetch("dkv", wdkv_hbm, wdkv)
    for i in range(n_q):
        fetch(i, wq_hbm.at[:, i * q_blk:(i + 1) * q_blk], wq.at[:, i * q_blk:(i + 1) * q_blk])
        if i == 0:
            fetch("uk", wuk_hbm, wuk)

    def cache_copy(i):
        rows_b = pl.ds(i * c_blk, c_blk)
        return pltpu.make_async_copy(cache_hbm.at[rows_b], cache.at[rows_b], c_sem.at[i])

    for i in range(seqs // c_blk):
        cache_copy(i).start()
    fetch("uv", wuv_hbm, wuv)
    fetch("o", wo_hbm, wo)

    while_loading()
    lane = lax.broadcasted_iota(jnp.int32, (seqs, rope), 1)
    freq = jnp.exp(lax.rem(lane, rope // 2).astype(jnp.float32) * (-2.0 * jnp.log(10000.0) / rope))
    row = lax.broadcasted_iota(jnp.int32, (seqs, rope), 0)
    pos = jnp.zeros((seqs, rope), jnp.int32)
    for b in range(seqs):
        pos = jnp.where(row == b, lens_ref[b], pos)
    angle = pos.astype(jnp.float32) * freq
    cos_t = jnp.cos(angle)
    sin_t = jnp.where(lane < rope // 2, -jnp.sin(angle), jnp.sin(angle))

    def rotate(u):
        swapped = jnp.concatenate([u[:, rope // 2:], u[:, :rope // 2]], axis=1)
        return u * cos_t + swapped * sin_t

    contract_last = (((1,), (1,)), ((), ()))
    x = x_ref[...]
    copies["dkv"].wait()
    raw = lax.dot_general(x, wdkv[...], contract_last, preferred_element_type=jnp.float32)
    lat = raw[:, :latent].astype(jnp.bfloat16)
    pe = rotate(raw[:, latent:latent + rope]).astype(jnp.bfloat16)
    kv_ref[:, :latent] = lat
    kv_ref[:, latent:latent + rope] = pe
    kv_rows[:, :latent] = lat.astype(jnp.float32)
    kv_rows[:, latent:latent + rope] = pe.astype(jnp.float32)

    n_lat = latent // LANES
    for p in range(heads // 2):
        if (p * pair) % q_blk == 0:
            copies[p * pair // q_blk].wait()
        if p == 0:
            copies["uk"].wait()
        qp = jnp.dot(x, wq[:, p * pair:(p + 1) * pair], preferred_element_type=jnp.float32).astype(jnp.bfloat16).astype(jnp.float32)
        for i in range(2):
            h = 2 * p + i
            base = i * (nope + rope)
            q_n = qp[:, base:base + nope].astype(jnp.bfloat16)
            q_lat = jnp.dot(q_n, wuk[h], preferred_element_type=jnp.float32)
            q_pe = rotate(qp[:, base + nope:base + nope + rope])
            q_lat = q_lat.astype(jnp.bfloat16).astype(jnp.float32)
            for t in range(n_lat):
                q_rows[t, h * seqs:(h + 1) * seqs, :] = q_lat[:, t * LANES:(t + 1) * LANES]
            q_rows[n_lat, h * seqs:(h + 1) * seqs, :rope] = q_pe.astype(jnp.bfloat16).astype(jnp.float32)

    scale = (nope + rope) ** -0.5
    keys = cache.shape[2]
    key_id = lax.broadcasted_iota(jnp.int32, (heads, keys), 1)

    def attend(i, carry):
        cache_copy(i).wait()
        ids = [i * c_blk + j for j in range(c_blk)]
        qs = [[q_rows[t, pl.ds(b, heads, stride=seqs), :] for t in range(n_lat + 1)] for b in ids]
        s_old, s_new, kls = [], [], []
        for b, q in zip(ids, qs):
            ql, qr = jnp.concatenate(q[:n_lat], axis=1), q[n_lat][:, :rope]
            s_old.append(jnp.dot(ql.astype(jnp.bfloat16), cache[b, :latent, :], preferred_element_type=jnp.float32)
                         + jnp.dot(qr.astype(jnp.bfloat16), cache[b, latent:latent + rope, :], preferred_element_type=jnp.float32))
        for b, q in zip(ids, qs):
            kv = kv_rows[pl.ds(b, 1), :]
            prod = q[0] * kv[:, :LANES]
            for t in range(1, n_lat):
                prod += q[t] * kv[:, t * LANES:(t + 1) * LANES]
            s_new.append(jnp.sum(prod, axis=1, keepdims=True)
                         + jnp.sum(q[n_lat][:, :rope] * kv[:, latent:latent + rope], axis=1, keepdims=True))
            kls.append(kv[:, :latent])
        s_old = [jnp.where(key_id < lens_ref[b], s * scale, -jnp.inf) for b, s in zip(ids, s_old)]
        s_old = jnp.concatenate(s_old, axis=0)
        s_new = jnp.concatenate(s_new, axis=0) * scale
        top = jnp.maximum(jnp.max(s_old, axis=1, keepdims=True), s_new)
        e_old = jnp.exp(s_old - top)
        e_new = jnp.exp(s_new - top)
        total = jnp.sum(e_old, axis=1, keepdims=True) + e_new
        p_old = (e_old / total).astype(jnp.bfloat16)
        p_new = (e_new / total).astype(jnp.bfloat16).astype(jnp.float32)
        for j, b in enumerate(ids):
            hs = slice(j * heads, (j + 1) * heads)
            o = lax.dot_general(p_old[hs], cache[b, :latent, :], contract_last, preferred_element_type=jnp.float32) + p_new[hs] * kls[j]
            for t in range(n_lat):
                o_rows[t, pl.ds(b, heads, stride=seqs), :] = o[:, t * LANES:(t + 1) * LANES]
        return carry

    lax.fori_loop(0, seqs // c_blk, attend, 0)

    copies["uv"].wait()
    for h in range(heads):
        o = jnp.concatenate([o_rows[t, h * seqs:(h + 1) * seqs, :] for t in range(n_lat)], axis=1).astype(jnp.bfloat16)
        v_rows[:, h * v_dim:(h + 1) * v_dim] = jnp.dot(o, wuv[h], preferred_element_type=jnp.float32).astype(jnp.bfloat16)
    copies["o"].wait()
    for j in range(hidden // 256):
        cs = slice(j * 256, (j + 1) * 256)
        a = jnp.dot(v_rows[...], wo[:, cs], preferred_element_type=jnp.float32).astype(jnp.bfloat16)
        h_out[:, cs] = (x_ref[:, cs].astype(jnp.float32) + a.astype(jnp.float32)).astype(jnp.bfloat16)


def attention_scratch(seqs, hidden, heads, nope, latent, rope, v_dim, keys):
    bf = jnp.bfloat16
    wide = latent + LANES
    return [pltpu.VMEM((hidden, heads * (nope + rope)), bf), pltpu.VMEM((latent + rope, hidden), bf),
            pltpu.VMEM((heads, nope, latent), bf), pltpu.VMEM((heads, latent, v_dim), bf),
            pltpu.VMEM((heads * v_dim, hidden), bf), pltpu.VMEM((seqs, latent + rope, keys), bf),
            pltpu.VMEM((wide // LANES, heads * seqs, LANES), jnp.float32), pltpu.VMEM((seqs, wide), jnp.float32),
            pltpu.VMEM((latent // LANES, heads * seqs, LANES), jnp.float32), pltpu.VMEM((seqs, heads * v_dim), bf),
            pltpu.SemaphoreType.DMA((8,)), pltpu.SemaphoreType.DMA((2,))]


def chip_order(side):
    def hops(off):
        return sum(min(v, side - v) for v in off)

    offs = [(dx, dy) for dy in range(side) for dx in range(side)]
    return sorted(offs, key=lambda off: (hops(off), -max(min(v, side - v) for v in off), off))


def layer_kernel(n_dev, x_ref, lens_ref, routes_ref, gates_ref, cache_hbm, wq_hbm, wdkv_hbm, wuk_hbm, wuv_hbm, wo_hbm,
                 shg_hbm, shu_hbm, shd_hbm, exg_hbm, exu_hbm, exd_hbm, out_ref, kv_ref,
                 h_ref, oh_ref, gate_ref, h_all, oh_all, rows, act, y_buf, back, sh_acc,
                 ag_send, ag_recv, core_send, core_recv, oh_send_sem, oh_recv_sem, ret_send, ret_recv, local_sem):
    barrier = pltpu.get_barrier_semaphore()
    me = lax.axis_index("ep")
    for i in range(1, n_dev):
        pl.semaphore_signal(barrier, inc=1, device_id={"ep": lax.rem(me + i, n_dev)}, device_id_type=MESH)

    seqs, hidden = x_ref.shape
    heads, nope, latent = wuk_hbm.shape

    def attend(*scratch):
        attention(x_ref, lens_ref, cache_hbm, wq_hbm, wdkv_hbm, wuk_hbm, wuv_hbm, wo_hbm, kv_ref, h_ref, *scratch,
                  while_loading=lambda: slot_tables(n_dev, routes_ref, gates_ref, oh_ref, gate_ref))

    pl.run_scoped(attend, *attention_scratch(seqs, hidden, heads, nope, latent, wdkv_hbm.shape[0] - latent, wuv_hbm.shape[2], cache_hbm.shape[2]))

    def experts(*scratch):
        moe(n_dev, h_ref, oh_ref, gate_ref, shg_hbm, shu_hbm, shd_hbm, exg_hbm, exu_hbm, exd_hbm, out_ref,
            h_all, oh_all, rows, act, y_buf, back, *scratch[:-2], sh_acc,
            ag_send, ag_recv, core_send, core_recv, oh_send_sem, oh_recv_sem, ret_send, ret_recv, *scratch[-2:], local_sem)

    n_exp, _, ff = exg_hbm.shape
    n_ring, blk = 4, 256
    bf = jnp.bfloat16
    pl.run_scoped(
        experts,
        pltpu.VMEM((n_exp, hidden, ff), bf), pltpu.VMEM((n_exp, hidden, ff), bf), pltpu.VMEM((n_exp, ff, hidden), bf),
        pltpu.VMEM((n_ring, hidden, blk), bf), pltpu.VMEM((n_ring, hidden, blk), bf), pltpu.VMEM((n_ring, blk, hidden), bf),
        pltpu.SemaphoreType.DMA((n_exp * 3,)), pltpu.SemaphoreType.DMA((3, n_ring)))


def moe(n_dev, h_ref, oh_ref, gate_ref, shg_hbm, shu_hbm, shd_hbm, exg_hbm, exu_hbm, exd_hbm, out_ref,
        h_all, oh_all, rows, act, y_buf, back, wg, wu, wd, ring_g, ring_u, ring_d, sh_acc,
        ag_send, ag_recv, core_send, core_recv, oh_send_sem, oh_recv_sem, ret_send, ret_recv, w_sem, ring_sem, local_sem):
    side = int((n_dev // 2) ** 0.5)
    offs = chip_order(side)
    slot_of = {off: k for k, off in enumerate(offs)}
    n_chips = len(offs)
    me = lax.axis_index("ep")
    core = lax.rem(me, 2)
    my_x = lax.rem(me // 2, side)
    my_y = me // (2 * side)
    hidden = h_ref.shape[1]
    q4 = hidden // 4

    def device_at(off, c):
        return (lax.rem(my_y + off[1], side) * side + lax.rem(my_x + off[0], side)) * 2 + c

    def minus(a, b):
        return ((a[0] - b[0]) % side, (a[1] - b[1]) % side)

    partner = device_at((0, 0), 1 - core)

    n_exp = wg.shape[0]
    w_copies = []
    for e in range(n_exp):
        for m, (src, dst) in enumerate(((exg_hbm, wg), (exu_hbm, wu), (exd_hbm, wd))):
            cp = pltpu.make_async_copy(src.at[e], dst.at[e], w_sem.at[e * 3 + m])
            cp.start()
            w_copies.append(cp)
    n_ring, _, blk = ring_g.shape
    n_steps = shg_hbm.shape[1] // blk

    def ring_copies(step, slot):
        cols = pl.ds(pl.multiple_of(step * blk, blk), blk)
        return (pltpu.make_async_copy(shg_hbm.at[:, cols], ring_g.at[slot], ring_sem.at[0, slot]),
                pltpu.make_async_copy(shu_hbm.at[:, cols], ring_u.at[slot], ring_sem.at[1, slot]),
                pltpu.make_async_copy(shd_hbm.at[cols, :], ring_d.at[slot], ring_sem.at[2, slot]))

    for s in range(n_ring):
        for cp in ring_copies(s, s):
            cp.start()

    h_all[core] = h_ref[...]
    oh_all[core] = oh_ref[0, core]

    pl.semaphore_wait(pltpu.get_barrier_semaphore(), n_dev - 1)

    A, B, WHOLE = (0, 2), (2, 2), (0, 4)
    A1, A0, B0, B1 = (0, 1), (1, 1), (2, 1), (3, 1)
    xp, xm, yp, ym = (1, 0), (side - 1, 0), (0, 1), (0, side - 1)
    pieces, sends, core_pieces = {}, [], {}

    def cols_of(part):
        return pl.ds(part[0] * q4, part[1] * q4)

    def forward(off, part, d):
        dst_off = minus(off, d)
        n = len(pieces)
        src = h_ref if off == (0, 0) else h_all.at[slot_of[off] * 2 + core]
        cp = pltpu.make_async_remote_copy(
            src_ref=src.at[:, cols_of(part)], dst_ref=h_all.at[slot_of[dst_off] * 2 + core, :, cols_of(part)],
            send_sem=ag_send.at[n], recv_sem=ag_recv.at[n], device_id={"ep": device_at(d, core)}, device_id_type=MESH)
        cp.start()
        pieces[(dst_off, part)] = cp
        sends.append(cp)

    def to_partner(off, part):
        n = len(core_pieces)
        src = h_ref if off == (0, 0) else h_all.at[slot_of[off] * 2 + core]
        cp = pltpu.make_async_remote_copy(
            src_ref=src.at[:, cols_of(part)], dst_ref=h_all.at[slot_of[off] * 2 + core, :, cols_of(part)],
            send_sem=core_send.at[n], recv_sem=core_recv.at[n], device_id={"ep": partner}, device_id_type=MESH)
        cp.start()
        core_pieces[(off, part)] = cp
        sends.append(cp)

    def arrived(off, *parts):
        for part in parts:
            pieces[(off, part)].wait_recv()

    for d in (xp, xm):
        forward((0, 0), A, d)
    for d in (yp, ym):
        forward((0, 0), B, d)
    for d in (xp, xm):
        forward((0, 0), B, d)
    for d in (yp, ym):
        forward((0, 0), A, d)
    to_partner((0, 0), A)
    to_partner((0, 0), B)

    oh_copies = []
    for k, off in enumerate(offs):
        there = slot_of[minus((0, 0), off)]
        for c in ((None,) if k == 0 else (0, 1)):
            dst_core = 1 - core if c is None else c
            n = len(oh_copies)
            cp = pltpu.make_async_remote_copy(
                src_ref=oh_ref.at[there % 2, k * 2 + dst_core], dst_ref=oh_all.at[there * 2 + core],
                send_sem=oh_send_sem.at[n], recv_sem=oh_recv_sem.at[there * 2 + core],
                device_id={"ep": device_at(off, dst_core)}, device_id_type=MESH)
            cp.start()
            oh_copies.append(cp)
            sends.append(cp)

    for off, d, quarter in ((xm, xp, A0), (xp, xm, A1)):
        arrived(off, A)
        forward(off, A, yp)
        forward(off, A, ym)
        forward(off, quarter, d)
        to_partner(off, A)
    for off, d, quarter in ((ym, yp, B0), (yp, ym, B1)):
        arrived(off, B)
        forward(off, B, xp)
        forward(off, B, xm)
        forward(off, quarter, d)
        to_partner(off, B)
    for off, d, quarter in ((xm, xp, B0), (xp, xm, B1)):
        arrived(off, B)
        forward(off, quarter, d)
        to_partner(off, B)
    for off, d, quarter in ((ym, yp, A0), (yp, ym, A1)):
        arrived(off, A)
        forward(off, quarter, d)
        to_partner(off, A)
    x2, y2 = (2, 0), (0, 2)
    arrived(x2, A0, A1)
    forward(x2, A, yp)
    forward(x2, A, ym)
    to_partner(x2, A)
    arrived(y2, B0, B1)
    forward(y2, B, xp)
    forward(y2, B, xm)
    to_partner(y2, B)
    diagonals = [(dx, dy) for dy in (1, side - 1) for dx in (1, side - 1)]
    for off in diagonals:
        arrived(off, A)
        if off[1] == 1:
            forward(off, A1, ym)
        else:
            forward(off, A0, yp)
        to_partner(off, A)
        arrived(off, B)
        if off[0] == 1:
            forward(off, B1, xm)
        else:
            forward(off, B0, xp)
        to_partner(off, B)
    arrived(x2, B0, B1)
    to_partner(x2, B)
    arrived(y2, A0, A1)
    to_partner(y2, A)

    def hop3():
        for off, d, quarter in (((2, side - 1), yp, A0), ((2, 1), ym, A1)):
            arrived(off, A)
            forward(off, quarter, d)
            to_partner(off, A)
        for off, d, quarter in (((side - 1, 2), xp, B0), ((1, 2), xm, B1)):
            arrived(off, B)
            forward(off, quarter, d)
            to_partner(off, B)
        for off in ((2, side - 1), (2, 1)):
            arrived(off, B0, B1)
            to_partner(off, B)
        for off in ((side - 1, 2), (1, 2)):
            arrived(off, A0, A1)
            to_partner(off, A)

    def hop4():
        far = (2, 2)
        arrived(far, A0, A1)
        to_partner(far, A)
        arrived(far, B0, B1)
        to_partner(far, B)

    def ready(ks):
        for k in ks:
            for part in (A, B):
                core_pieces[(offs[k], part)].wait_recv()
            for c in ((1 - core,) if k == 0 else (0, 1)):
                pltpu.make_async_remote_copy(
                    src_ref=oh_ref.at[0, 0], dst_ref=oh_all.at[k * 2 + c], send_sem=oh_send_sem.at[0],
                    recv_sem=oh_recv_sem.at[k * 2 + c], device_id={"ep": partner}, device_id_type=MESH).wait_recv()

    half = n_chips // 2
    n_src = half * 2
    n_row = n_src * SLOTS_EXP
    seqs = h_ref.shape[0]
    ff = wg.shape[2]

    def gather_rows(k0):
        for g in range(half // 2):
            s0 = k0 * 2 + g * 4
            table = oh_all[s0:s0 + 4].reshape(4 * 2 * SLOTS_EXP, LANES)
            got = jnp.dot(table, h_all[s0:s0 + 4].reshape(4 * seqs, hidden), preferred_element_type=jnp.float32)
            got = got.reshape(4, n_exp, SLOTS_EXP, hidden)
            for e in range(n_exp):
                rows[e, g * 4 * SLOTS_EXP:(g + 1) * 4 * SLOTS_EXP, :] = got[:, e].reshape(4 * SLOTS_EXP, hidden).astype(jnp.bfloat16)

    def gate_up(e):
        r = rows.at[e]
        full = ff // 256
        for j in range(full):
            cs = slice(j * 256, (j + 1) * 256)
            g = jnp.dot(r[...], wg[e, :, cs], preferred_element_type=jnp.float32)
            u = jnp.dot(r[...], wu[e, :, cs], preferred_element_type=jnp.float32)
            act[e, :, cs] = (jax.nn.silu(g) * u).astype(jnp.bfloat16)
        if ff % 256:
            cs = slice(full * 256, ff)
            wid = ff - full * 256
            both = jnp.dot(r[...], jnp.concatenate([wg[e, :, cs], wu[e, :, cs]], axis=1), preferred_element_type=jnp.float32)
            act[e, :, cs] = (jax.nn.silu(both[:, :wid]) * both[:, wid:]).astype(jnp.bfloat16)

    def down(k0, part):
        for j in range(part[0] * q4 // 256, (part[0] + part[1]) * q4 // 256):
            cs = slice(j * 256, (j + 1) * 256)
            outs = [jnp.dot(act[e], wd[e, :, cs], preferred_element_type=jnp.float32).reshape(n_src, 1, SLOTS_EXP, 256) for e in range(n_exp)]
            y_buf[k0 * 2:k0 * 2 + n_src, :, cs] = jnp.concatenate(outs, axis=1).reshape(n_src, n_exp * SLOTS_EXP, 256).astype(jnp.bfloat16)

    ret_count = [0]

    def give_back(ks, parts):
        for part in parts:
            for k in ks:
                back_k = slot_of[minus((0, 0), offs[k])]
                k1, back_k1 = (back_k, k) if back_k in ks else (k, back_k)
                place = k + core * (k1 - k)
                there = back_k + core * (back_k1 - back_k)
                off = tuple(offs[k][a] + core * (offs[k1][a] - offs[k][a]) for a in range(2))
                for c in ((None,) if k == 0 else (0, 1)):
                    dst_core = 1 - core if c is None else c
                    cp = pltpu.make_async_remote_copy(
                        src_ref=y_buf.at[place * 2 + dst_core, :, cols_of(part)],
                        dst_ref=back.at[there * 2 + core, :, cols_of(part)],
                        send_sem=ret_send.at[ret_count[0]], recv_sem=ret_recv.at[(there * 2 + core) * 2 + part[0] // 2],
                        device_id={"ep": device_at(off, dst_core)}, device_id_type=MESH)
                    cp.start()
                    ret_count[0] += 1
                    sends.append(cp)

    near, far = list(range(half)), list(range(half, n_chips))
    ready(near)
    gather_rows(0)
    for e in range(n_exp):
        w_copies[e * 3].wait()
        w_copies[e * 3 + 1].wait()
        gate_up(e)
        if e == 0:
            hop3()
    for e in range(n_exp):
        w_copies[e * 3 + 2].wait()
    hop4()
    down(0, WHOLE)
    own = pltpu.make_async_copy(y_buf.at[core], back.at[core], local_sem)
    own.start()
    give_back(near[::-1], (WHOLE,))

    ready(far)
    gather_rows(half)

    def far_gate_up(e, carry):
        gate_up(e)
        return carry

    lax.fori_loop(0, n_exp, far_gate_up, 0)
    for part in (A, B):
        down(half, part)
        give_back(far[::-1], (part,))

    sh_acc[...] = jnp.zeros_like(sh_acc)

    def shared_step(i, carry):
        slot = lax.rem(i, n_ring)
        for cp in ring_copies(i, slot):
            cp.wait()
        g = jnp.dot(h_ref[...], ring_g[slot], preferred_element_type=jnp.float32)
        u = jnp.dot(h_ref[...], ring_u[slot], preferred_element_type=jnp.float32)
        a = (jax.nn.silu(g) * u).astype(jnp.bfloat16)
        sh_acc[...] += jnp.dot(a, ring_d[slot], preferred_element_type=jnp.float32)

        @pl.when(i + n_ring < n_steps)
        def _():
            for cp in ring_copies(i + n_ring, slot):
                cp.start()

        return carry

    lax.fori_loop(0, n_steps, shared_step, 0)

    own.wait()

    def returned(k, part):
        for c in ((1 - core,) if k == 0 else (0, 1)):
            pltpu.make_async_remote_copy(
                src_ref=y_buf.at[0, :, cols_of(part)], dst_ref=back.at[k * 2 + c, :, cols_of(part)], send_sem=ret_send.at[0],
                recv_sem=ret_recv.at[(k * 2 + c) * 2 + part[0] // 2], device_id={"ep": partner}, device_id_type=MESH).wait_recv()

    from_near = [slot_of[minus((0, 0), offs[k])] for k in near]
    for k in from_near:
        returned(k, WHOLE)
    n_slot = n_chips * 2 * n_exp * SLOTS_EXP
    for j in range(hidden // 256):
        if j * 256 % (2 * q4) == 0:
            for k in range(n_chips):
                if k not in from_near:
                    returned(k, A if j == 0 else B)
        cs = slice(j * 256, (j + 1) * 256)
        part = lax.dot_general(gate_ref[...], back[:, :, cs].reshape(n_slot, 256), (((0,), (0,)), ((), ())), preferred_element_type=jnp.float32)
        routed = part[:seqs] + part[seqs:2 * seqs] + part[2 * seqs:3 * seqs]
        shared = sh_acc[:, cs].astype(jnp.bfloat16).astype(jnp.float32)
        out_ref[:, cs] = (h_ref[:, cs].astype(jnp.float32) + shared + routed).astype(jnp.bfloat16)
    for cp in sends:
        cp.wait_send()


def slot_tables(n_dev, routes_ref, gates_ref, oh_ref, gate_ref):
    side = int((n_dev // 2) ** 0.5)
    me = lax.axis_index("ep")
    core, my_x, my_y = lax.rem(me, 2), lax.rem(me // 2, side), me // (2 * side)
    top_k, seqs = routes_ref.shape
    per_chip = oh_ref.shape[1] * oh_ref.shape[2] // (n_dev // 2)
    row = lax.broadcasted_iota(jnp.int32, (per_chip, LANES), 0)
    exp_chip = per_chip // SLOTS_EXP
    ids = jnp.concatenate([
        row // SLOTS_EXP + exp_chip * (lax.rem(my_y + dy, side) * side + lax.rem(my_x + dx, side))
        for dx, dy in chip_order(side)], axis=0)
    n_slot = ids.shape[0]
    pos = lax.rem(lax.broadcasted_iota(jnp.int32, (n_slot, LANES), 0), SLOTS_EXP)
    block = lax.broadcasted_iota(jnp.int32, (n_slot, LANES), 1) // seqs
    routes = jnp.concatenate([routes_ref[...]] * (LANES // seqs), axis=1)
    gates = jnp.concatenate([gates_ref[...]] * (LANES // seqs), axis=1)
    has = jnp.zeros((n_slot, LANES), jnp.float32)
    gate = jnp.zeros((n_slot, LANES), jnp.float32)
    for k in range(top_k):
        hit = ids == routes[k:k + 1, :]
        has = jnp.where(hit, 1.0, has)
        gate = jnp.where(hit, gates[k:k + 1, :], gate)
    src = lax.broadcasted_iota(jnp.int32, (LANES, LANES), 0)
    dst = lax.broadcasted_iota(jnp.int32, (LANES, LANES), 1)
    earlier = jnp.where((src < dst) & (src // seqs == dst // seqs), 1.0, 0.0).astype(jnp.bfloat16)
    rank = jnp.dot(has.astype(jnp.bfloat16), earlier, preferred_element_type=jnp.float32)
    sel = jnp.where(rank == pos.astype(jnp.float32), has, 0.0)
    for v in range(2):
        oh_ref[v] = jnp.where(block == 2 * v + core, sel, 0.0).astype(jnp.bfloat16).reshape(oh_ref.shape[1:])
    gate = gate * sel
    g0 = gate.astype(jnp.bfloat16).astype(jnp.float32)
    g1 = (gate - g0).astype(jnp.bfloat16).astype(jnp.float32)
    g2 = gate - g0 - g1
    gate_ref[...] = jnp.where(block == 0, g0, jnp.where(block == 1, g1, jnp.where(block == 2, g2, 0.0))).astype(jnp.bfloat16)


def solution(mesh):
    n_dev = mesh.shape["ep"]

    def device_step(x_blk, cache_blk, len_blk, routes, route_gates, w_q, w_dkv, w_uk, w_uv, w_o, sh_gate, sh_up, sh_down, ex_gate, ex_up, ex_down):
        seqs, hidden = x_blk.shape
        n_exp, _, ff = ex_gate.shape
        n_chips = n_dev // 2
        slots = n_exp * SLOTS_EXP
        half_rows = n_chips * SLOTS_EXP
        bf = jnp.bfloat16
        dma = pltpu.SemaphoreType.DMA
        vmem = pl.BlockSpec(memory_space=pltpu.VMEM)
        hbm = pl.BlockSpec(memory_space=pl.ANY)
        layer_out, kv_row = pl.pallas_call(
            functools.partial(layer_kernel, n_dev),
            out_shape=(jax.ShapeDtypeStruct((seqs, hidden), bf), jax.ShapeDtypeStruct((seqs, w_dkv.shape[1]), bf)),
            in_specs=[vmem, pl.BlockSpec(memory_space=pltpu.SMEM), vmem, vmem] + [hbm] * 12,
            out_specs=(vmem, vmem),
            scratch_shapes=[
                pltpu.VMEM((seqs, hidden), bf),
                pltpu.VMEM((2, n_dev, slots, LANES), bf),
                pltpu.VMEM((n_dev * slots, LANES), bf),
                pltpu.VMEM((n_dev, seqs, hidden), bf),
                pltpu.VMEM((n_dev, slots, LANES), bf),
                pltpu.VMEM((n_exp, half_rows, hidden), bf),
                pltpu.VMEM((n_exp, half_rows, ff), bf),
                pltpu.VMEM((n_dev, slots, hidden), bf),
                pltpu.VMEM((n_dev, slots, hidden), bf),
                pltpu.VMEM((seqs, hidden), jnp.float32),
                dma((64,)), dma((64,)), dma((2 * n_chips,)), dma((2 * n_chips,)),
                dma((n_dev,)), dma((n_dev,)), dma((2 * n_dev,)), dma((2 * n_dev,)), dma,
            ],
            compiler_params=pltpu.CompilerParams(collective_id=0, has_side_effects=True, vmem_limit_bytes=67043328),
        )(x_blk, len_blk, routes.T, route_gates.T, cache_blk.transpose(0, 2, 1), w_q, w_dkv.T, w_uk, w_uv, w_o,
          sh_gate, sh_up, sh_down, ex_gate, ex_up, ex_down)
        return layer_out, kv_row

    batch_spec = P(("dp", "ep"))
    weight_spec = P()
    expert_spec = P("ep")
    in_specs = (batch_spec,) * 5 + (weight_spec,) * 8 + (expert_spec,) * 3
    return jax.shard_map(device_step, mesh=mesh, in_specs=in_specs, out_specs=(batch_spec, batch_spec), check_vma=False)
```

```python
import functools

import jax
import jax.numpy as jnp
from jax import lax
from jax.experimental import pallas as pl
from jax.experimental.pallas import tpu as pltpu
from jax.sharding import PartitionSpec as P

MESH = pl.DeviceIdType.MESH
SLOTS_EXP = 8
LANES = 128

def attention(x_ref, lens_ref, cache_hbm, wq_hbm, wdkv_hbm, wuk_hbm, wuv_hbm, wo_hbm, kv_ref, h_out,
              wq, wdkv, wuk, wuv, wo, cache, q_rows, kv_rows, o_rows, v_rows, a_sem, c_sem, while_loading):
    seqs, hidden = x_ref.shape
    heads, nope, latent = wuk.shape
    rope = wdkv.shape[0] - latent
    v_dim = wuv.shape[2]
    pair = 2 * (nope + rope)
    n_q = 4
    q_blk = wq.shape[1] // n_q
    c_blk = seqs // c_sem.shape[0]
    copies = {}

    def fetch(name, src, dst):
        cp = pltpu.make_async_copy(src, dst, a_sem.at[len(copies)])
        cp.start()
        copies[name] = cp

    fetch("dkv", wdkv_hbm, wdkv)
    for i in range(n_q):
        fetch(i, wq_hbm.at[:, i * q_blk:(i + 1) * q_blk], wq.at[:, i * q_blk:(i + 1) * q_blk])
        if i == 0:
            fetch("uk", wuk_hbm, wuk)

    def cache_copy(i):
        rows_b = pl.ds(i * c_blk, c_blk)
        return pltpu.make_async_copy(cache_hbm.at[rows_b], cache.at[rows_b], c_sem.at[i])

    for i in range(seqs // c_blk):
        cache_copy(i).start()
    fetch("uv", wuv_hbm, wuv)
    fetch("o", wo_hbm, wo)

    while_loading()
    lane = lax.broadcasted_iota(jnp.int32, (seqs, rope), 1)
    freq = jnp.exp(lax.rem(lane, rope // 2).astype(jnp.float32) * (-2.0 * jnp.log(10000.0) / rope))
    row = lax.broadcasted_iota(jnp.int32, (seqs, rope), 0)
    pos = jnp.zeros((seqs, rope), jnp.int32)
    for b in range(seqs):
        pos = jnp.where(row == b, lens_ref[b], pos)
    angle = pos.astype(jnp.float32) * freq
    cos_t = jnp.cos(angle)
    sin_t = jnp.where(lane < rope // 2, -jnp.sin(angle), jnp.sin(angle))

    def rotate(u):
        swapped = jnp.concatenate([u[:, rope // 2:], u[:, :rope // 2]], axis=1)
        return u * cos_t + swapped * sin_t

    contract_last = (((1,), (1,)), ((), ()))
    x = x_ref[...]
    copies["dkv"].wait()
    raw = lax.dot_general(x, wdkv[...], contract_last, preferred_element_type=jnp.float32)
    lat = raw[:, :latent].astype(jnp.bfloat16)
    pe = rotate(raw[:, latent:latent + rope]).astype(jnp.bfloat16)
    kv_ref[:, :latent] = lat
    kv_ref[:, latent:latent + rope] = pe
    kv_rows[:, :latent] = lat.astype(jnp.float32)
    kv_rows[:, latent:latent + rope] = pe.astype(jnp.float32)

    n_lat = latent // LANES
    for p in range(heads // 2):
        if (p * pair) % q_blk == 0:
            copies[p * pair // q_blk].wait()
        if p == 0:
            copies["uk"].wait()
        qp = jnp.dot(x, wq[:, p * pair:(p + 1) * pair], preferred_element_type=jnp.float32).astype(jnp.bfloat16).astype(jnp.float32)
        for i in range(2):
            h = 2 * p + i
            base = i * (nope + rope)
            q_n = qp[:, base:base + nope].astype(jnp.bfloat16)
            q_lat = jnp.dot(q_n, wuk[h], preferred_element_type=jnp.float32)
            q_pe = rotate(qp[:, base + nope:base + nope + rope])
            q_lat = q_lat.astype(jnp.bfloat16).astype(jnp.float32)
            for t in range(n_lat):
                q_rows[t, h * seqs:(h + 1) * seqs, :] = q_lat[:, t * LANES:(t + 1) * LANES]
            q_rows[n_lat, h * seqs:(h + 1) * seqs, :rope] = q_pe.astype(jnp.bfloat16).astype(jnp.float32)

    scale = (nope + rope) ** -0.5
    keys = cache.shape[2]
    key_id = lax.broadcasted_iota(jnp.int32, (heads, keys), 1)

    def attend(i, carry):
        cache_copy(i).wait()
        ids = [i * c_blk + j for j in range(c_blk)]
        qs = [[q_rows[t, pl.ds(b, heads, stride=seqs), :] for t in range(n_lat + 1)] for b in ids]
        s_old, s_new, kls = [], [], []
        for b, q in zip(ids, qs):
            ql, qr = jnp.concatenate(q[:n_lat], axis=1), q[n_lat][:, :rope]
            s_old.append(jnp.dot(ql.astype(jnp.bfloat16), cache[b, :latent, :], preferred_element_type=jnp.float32)
                         + jnp.dot(qr.astype(jnp.bfloat16), cache[b, latent:latent + rope, :], preferred_element_type=jnp.float32))
        for b, q in zip(ids, qs):
            kv = kv_rows[pl.ds(b, 1), :]
            prod = q[0] * kv[:, :LANES]
            for t in range(1, n_lat):
                prod += q[t] * kv[:, t * LANES:(t + 1) * LANES]
            s_new.append(jnp.sum(prod, axis=1, keepdims=True)
                         + jnp.sum(q[n_lat][:, :rope] * kv[:, latent:latent + rope], axis=1, keepdims=True))
            kls.append(kv[:, :latent])
        s_old = [jnp.where(key_id < lens_ref[b], s * scale, -jnp.inf) for b, s in zip(ids, s_old)]
        s_old = jnp.concatenate(s_old, axis=0)
        s_new = jnp.concatenate(s_new, axis=0) * scale
        top = jnp.maximum(jnp.max(s_old, axis=1, keepdims=True), s_new)
        e_old = jnp.exp(s_old - top)
        e_new = jnp.exp(s_new - top)
        total = jnp.sum(e_old, axis=1, keepdims=True) + e_new
        p_old = (e_old / total).astype(jnp.bfloat16)
        p_new = (e_new / total).astype(jnp.bfloat16).astype(jnp.float32)
        for j, b in enumerate(ids):
            hs = slice(j * heads, (j + 1) * heads)
            o = lax.dot_general(p_old[hs], cache[b, :latent, :], contract_last, preferred_element_type=jnp.float32) + p_new[hs] * kls[j]
            for t in range(n_lat):
                o_rows[t, pl.ds(b, heads, stride=seqs), :] = o[:, t * LANES:(t + 1) * LANES]
        return carry

    lax.fori_loop(0, seqs // c_blk, attend, 0)

    copies["uv"].wait()
    for h in range(heads):
        o = jnp.concatenate([o_rows[t, h * seqs:(h + 1) * seqs, :] for t in range(n_lat)], axis=1).astype(jnp.bfloat16)
        v_rows[:, h * v_dim:(h + 1) * v_dim] = jnp.dot(o, wuv[h], preferred_element_type=jnp.float32).astype(jnp.bfloat16)
    copies["o"].wait()
    for j in range(hidden // 256):
        cs = slice(j * 256, (j + 1) * 256)
        a = jnp.dot(v_rows[...], wo[:, cs], preferred_element_type=jnp.float32).astype(jnp.bfloat16)
        h_out[:, cs] = (x_ref[:, cs].astype(jnp.float32) + a.astype(jnp.float32)).astype(jnp.bfloat16)


def attention_scratch(seqs, hidden, heads, nope, latent, rope, v_dim, keys):
    bf = jnp.bfloat16
    wide = latent + LANES
    return [pltpu.VMEM((hidden, heads * (nope + rope)), bf), pltpu.VMEM((latent + rope, hidden), bf),
            pltpu.VMEM((heads, nope, latent), bf), pltpu.VMEM((heads, latent, v_dim), bf),
            pltpu.VMEM((heads * v_dim, hidden), bf), pltpu.VMEM((seqs, latent + rope, keys), bf),
            pltpu.VMEM((wide // LANES, heads * seqs, LANES), jnp.float32), pltpu.VMEM((seqs, wide), jnp.float32),
            pltpu.VMEM((latent // LANES, heads * seqs, LANES), jnp.float32), pltpu.VMEM((seqs, heads * v_dim), bf),
            pltpu.SemaphoreType.DMA((8,)), pltpu.SemaphoreType.DMA((2,))]


def chip_order(side):
    def hops(off):
        return sum(min(v, side - v) for v in off)

    offs = [(dx, dy) for dy in range(side) for dx in range(side)]
    return sorted(offs, key=lambda off: (hops(off), -max(min(v, side - v) for v in off), off))


def layer_kernel(n_dev, x_ref, lens_ref, routes_ref, gates_ref, cache_hbm, wq_hbm, wdkv_hbm, wuk_hbm, wuv_hbm, wo_hbm,
                 shg_hbm, shu_hbm, shd_hbm, exg_hbm, exu_hbm, exd_hbm, out_ref, kv_ref,
                 h_ref, oh_ref, gate_ref, h_all, oh_all, rows, act, y_buf, back, sh_acc,
                 ag_send, ag_recv, core_send, core_recv, oh_send_sem, oh_recv_sem, ret_send, ret_recv, local_sem):
    barrier = pltpu.get_barrier_semaphore()
    me = lax.axis_index("ep")
    for i in range(1, n_dev):
        pl.semaphore_signal(barrier, inc=1, device_id={"ep": lax.rem(me + i, n_dev)}, device_id_type=MESH)

    seqs, hidden = x_ref.shape
    heads, nope, latent = wuk_hbm.shape

    def attend(*scratch):
        attention(x_ref, lens_ref, cache_hbm, wq_hbm, wdkv_hbm, wuk_hbm, wuv_hbm, wo_hbm, kv_ref, h_ref, *scratch,
                  while_loading=lambda: slot_tables(n_dev, routes_ref, gates_ref, oh_ref, gate_ref))

    pl.run_scoped(attend, *attention_scratch(seqs, hidden, heads, nope, latent, wdkv_hbm.shape[0] - latent, wuv_hbm.shape[2], cache_hbm.shape[2]))

    def experts(*scratch):
        moe(n_dev, h_ref, oh_ref, gate_ref, shg_hbm, shu_hbm, shd_hbm, exg_hbm, exu_hbm, exd_hbm, out_ref,
            h_all, oh_all, rows, act, y_buf, back, *scratch[:-2], sh_acc,
            ag_send, ag_recv, core_send, core_recv, oh_send_sem, oh_recv_sem, ret_send, ret_recv, *scratch[-2:], local_sem)

    n_exp, _, ff = exg_hbm.shape
    n_ring, blk = 4, 256
    bf = jnp.bfloat16
    pl.run_scoped(
        experts,
        pltpu.VMEM((n_exp, hidden, ff), bf), pltpu.VMEM((n_exp, hidden, ff), bf), pltpu.VMEM((n_exp, ff, hidden), bf),
        pltpu.VMEM((n_ring, hidden, blk), bf), pltpu.VMEM((n_ring, hidden, blk), bf), pltpu.VMEM((n_ring, blk, hidden), bf),
        pltpu.SemaphoreType.DMA((n_exp * 3,)), pltpu.SemaphoreType.DMA((3, n_ring)))


def moe(n_dev, h_ref, oh_ref, gate_ref, shg_hbm, shu_hbm, shd_hbm, exg_hbm, exu_hbm, exd_hbm, out_ref,
        h_all, oh_all, rows, act, y_buf, back, wg, wu, wd, ring_g, ring_u, ring_d, sh_acc,
        ag_send, ag_recv, core_send, core_recv, oh_send_sem, oh_recv_sem, ret_send, ret_recv, w_sem, ring_sem, local_sem):
    side = int((n_dev // 2) ** 0.5)
    offs = chip_order(side)
    slot_of = {off: k for k, off in enumerate(offs)}
    n_chips = len(offs)
    me = lax.axis_index("ep")
    core = lax.rem(me, 2)
    my_x = lax.rem(me // 2, side)
    my_y = me // (2 * side)
    hidden = h_ref.shape[1]
    q4 = hidden // 4

    def device_at(off, c):
        return (lax.rem(my_y + off[1], side) * side + lax.rem(my_x + off[0], side)) * 2 + c

    def minus(a, b):
        return ((a[0] - b[0]) % side, (a[1] - b[1]) % side)

    partner = device_at((0, 0), 1 - core)

    n_exp = wg.shape[0]
    w_copies = []
    for e in range(n_exp):
        for m, (src, dst) in enumerate(((exg_hbm, wg), (exu_hbm, wu), (exd_hbm, wd))):
            cp = pltpu.make_async_copy(src.at[e], dst.at[e], w_sem.at[e * 3 + m])
            cp.start()
            w_copies.append(cp)
    n_ring, _, blk = ring_g.shape
    n_steps = shg_hbm.shape[1] // blk

    def ring_copies(step, slot):
        cols = pl.ds(pl.multiple_of(step * blk, blk), blk)
        return (pltpu.make_async_copy(shg_hbm.at[:, cols], ring_g.at[slot], ring_sem.at[0, slot]),
                pltpu.make_async_copy(shu_hbm.at[:, cols], ring_u.at[slot], ring_sem.at[1, slot]),
                pltpu.make_async_copy(shd_hbm.at[cols, :], ring_d.at[slot], ring_sem.at[2, slot]))

    for s in range(n_ring):
        for cp in ring_copies(s, s):
            cp.start()

    h_all[core] = h_ref[...]
    oh_all[core] = oh_ref[0, core]

    pl.semaphore_wait(pltpu.get_barrier_semaphore(), n_dev - 1)

    A, B, WHOLE = (0, 2), (2, 2), (0, 4)
    A1, A0, B0, B1 = (0, 1), (1, 1), (2, 1), (3, 1)
    xp, xm, yp, ym = (1, 0), (side - 1, 0), (0, 1), (0, side - 1)
    pieces, sends, core_pieces = {}, [], {}

    def cols_of(part):
        return pl.ds(part[0] * q4, part[1] * q4)

    def forward(off, part, d):
        dst_off = minus(off, d)
        n = len(pieces)
        src = h_ref if off == (0, 0) else h_all.at[slot_of[off] * 2 + core]
        cp = pltpu.make_async_remote_copy(
            src_ref=src.at[:, cols_of(part)], dst_ref=h_all.at[slot_of[dst_off] * 2 + core, :, cols_of(part)],
            send_sem=ag_send.at[n], recv_sem=ag_recv.at[n], device_id={"ep": device_at(d, core)}, device_id_type=MESH)
        cp.start()
        pieces[(dst_off, part)] = cp
        sends.append(cp)

    def to_partner(off, part):
        n = len(core_pieces)
        src = h_ref if off == (0, 0) else h_all.at[slot_of[off] * 2 + core]
        cp = pltpu.make_async_remote_copy(
            src_ref=src.at[:, cols_of(part)], dst_ref=h_all.at[slot_of[off] * 2 + core, :, cols_of(part)],
            send_sem=core_send.at[n], recv_sem=core_recv.at[n], device_id={"ep": partner}, device_id_type=MESH)
        cp.start()
        core_pieces[(off, part)] = cp
        sends.append(cp)

    def arrived(off, *parts):
        for part in parts:
            pieces[(off, part)].wait_recv()

    for d in (xp, xm):
        forward((0, 0), A, d)
    for d in (yp, ym):
        forward((0, 0), B, d)
    for d in (xp, xm):
        forward((0, 0), B, d)
    for d in (yp, ym):
        forward((0, 0), A, d)
    to_partner((0, 0), A)
    to_partner((0, 0), B)

    oh_copies = []
    for k, off in enumerate(offs):
        there = slot_of[minus((0, 0), off)]
        for c in ((None,) if k == 0 else (0, 1)):
            dst_core = 1 - core if c is None else c
            n = len(oh_copies)
            cp = pltpu.make_async_remote_copy(
                src_ref=oh_ref.at[there % 2, k * 2 + dst_core], dst_ref=oh_all.at[there * 2 + core],
                send_sem=oh_send_sem.at[n], recv_sem=oh_recv_sem.at[there * 2 + core],
                device_id={"ep": device_at(off, dst_core)}, device_id_type=MESH)
            cp.start()
            oh_copies.append(cp)
            sends.append(cp)

    for off, d, quarter in ((xm, xp, A0), (xp, xm, A1)):
        arrived(off, A)
        forward(off, A, yp)
        forward(off, A, ym)
        forward(off, quarter, d)
        to_partner(off, A)
    for off, d, quarter in ((ym, yp, B0), (yp, ym, B1)):
        arrived(off, B)
        forward(off, B, xp)
        forward(off, B, xm)
        forward(off, quarter, d)
        to_partner(off, B)
    for off, d, quarter in ((xm, xp, B0), (xp, xm, B1)):
        arrived(off, B)
        forward(off, quarter, d)
        to_partner(off, B)
    for off, d, quarter in ((ym, yp, A0), (yp, ym, A1)):
        arrived(off, A)
        forward(off, quarter, d)
        to_partner(off, A)
    x2, y2 = (2, 0), (0, 2)
    arrived(x2, A0, A1)
    forward(x2, A, yp)
    forward(x2, A, ym)
    forward(x2, A, y2)
    to_partner(x2, A)
    arrived(y2, B0, B1)
    forward(y2, B, xp)
    forward(y2, B, xm)
    forward(y2, B, x2)
    to_partner(y2, B)
    diagonals = [(dx, dy) for dy in (1, side - 1) for dx in (1, side - 1)]
    for off in diagonals:
        arrived(off, A)
        if off[1] == 1:
            forward(off, A1, ym)
        else:
            forward(off, A0, yp)
        to_partner(off, A)
        arrived(off, B)
        if off[0] == 1:
            forward(off, B1, xm)
        else:
            forward(off, B0, xp)
        to_partner(off, B)
    arrived(x2, B0, B1)
    to_partner(x2, B)
    arrived(y2, A0, A1)
    to_partner(y2, A)

    def hop3():
        for off in ((2, side - 1), (2, 1)):
            arrived(off, A)
            to_partner(off, A)
        for off in ((side - 1, 2), (1, 2)):
            arrived(off, B)
            to_partner(off, B)
        for off in ((2, side - 1), (2, 1)):
            arrived(off, B0, B1)
            to_partner(off, B)
        for off in ((side - 1, 2), (1, 2)):
            arrived(off, A0, A1)
            to_partner(off, A)

    def hop4():
        for part in (A, B):
            arrived((2, 2), part)
            to_partner((2, 2), part)

    def ready(ks):
        for k in ks:
            for part in (A, B):
                core_pieces[(offs[k], part)].wait_recv()
            for c in ((1 - core,) if k == 0 else (0, 1)):
                pltpu.make_async_remote_copy(
                    src_ref=oh_ref.at[0, 0], dst_ref=oh_all.at[k * 2 + c], send_sem=oh_send_sem.at[0],
                    recv_sem=oh_recv_sem.at[k * 2 + c], device_id={"ep": partner}, device_id_type=MESH).wait_recv()

    half = n_chips // 2
    n_src = half * 2
    n_row = n_src * SLOTS_EXP
    seqs = h_ref.shape[0]
    ff = wg.shape[2]

    def gather_rows(k0):
        for g in range(half // 2):
            s0 = k0 * 2 + g * 4
            table = oh_all[s0:s0 + 4].reshape(4 * 2 * SLOTS_EXP, LANES)
            got = jnp.dot(table, h_all[s0:s0 + 4].reshape(4 * seqs, hidden), preferred_element_type=jnp.float32)
            got = got.reshape(4, n_exp, SLOTS_EXP, hidden)
            for e in range(n_exp):
                rows[e, g * 4 * SLOTS_EXP:(g + 1) * 4 * SLOTS_EXP, :] = got[:, e].reshape(4 * SLOTS_EXP, hidden).astype(jnp.bfloat16)

    def gate_up(e):
        r = rows.at[e]
        full = ff // 256
        for j in range(full):
            cs = slice(j * 256, (j + 1) * 256)
            g = jnp.dot(r[...], wg[e, :, cs], preferred_element_type=jnp.float32)
            u = jnp.dot(r[...], wu[e, :, cs], preferred_element_type=jnp.float32)
            act[e, :, cs] = (jax.nn.silu(g) * u).astype(jnp.bfloat16)
        if ff % 256:
            cs = slice(full * 256, ff)
            wid = ff - full * 256
            both = jnp.dot(r[...], jnp.concatenate([wg[e, :, cs], wu[e, :, cs]], axis=1), preferred_element_type=jnp.float32)
            act[e, :, cs] = (jax.nn.silu(both[:, :wid]) * both[:, wid:]).astype(jnp.bfloat16)

    def down(k0, part):
        for j in range(part[0] * q4 // 256, (part[0] + part[1]) * q4 // 256):
            cs = slice(j * 256, (j + 1) * 256)
            outs = [jnp.dot(act[e], wd[e, :, cs], preferred_element_type=jnp.float32).reshape(n_src, 1, SLOTS_EXP, 256) for e in range(n_exp)]
            y_buf[k0 * 2:k0 * 2 + n_src, :, cs] = jnp.concatenate(outs, axis=1).reshape(n_src, n_exp * SLOTS_EXP, 256).astype(jnp.bfloat16)

    ret_count = [0]

    def give_back(ks, parts):
        for part in parts:
            for k in ks:
                back_k = slot_of[minus((0, 0), offs[k])]
                k1, back_k1 = (back_k, k) if back_k in ks else (k, back_k)
                place = k + core * (k1 - k)
                there = back_k + core * (back_k1 - back_k)
                off = tuple(offs[k][a] + core * (offs[k1][a] - offs[k][a]) for a in range(2))
                for c in ((None,) if k == 0 else (0, 1)):
                    dst_core = 1 - core if c is None else c
                    cp = pltpu.make_async_remote_copy(
                        src_ref=y_buf.at[place * 2 + dst_core, :, cols_of(part)],
                        dst_ref=back.at[there * 2 + core, :, cols_of(part)],
                        send_sem=ret_send.at[ret_count[0]], recv_sem=ret_recv.at[(there * 2 + core) * 2 + part[0] // 2],
                        device_id={"ep": device_at(off, dst_core)}, device_id_type=MESH)
                    cp.start()
                    ret_count[0] += 1
                    sends.append(cp)

    near, far = list(range(half)), list(range(half, n_chips))
    ready(near)
    gather_rows(0)
    for e in range(n_exp):
        w_copies[e * 3].wait()
        w_copies[e * 3 + 1].wait()
        gate_up(e)
        if e == 0:
            hop3()
    for e in range(n_exp):
        w_copies[e * 3 + 2].wait()
    hop4()
    down(0, WHOLE)
    own = pltpu.make_async_copy(y_buf.at[core], back.at[core], local_sem)
    own.start()
    give_back(near[::-1], (WHOLE,))

    ready(far)
    gather_rows(half)

    def far_gate_up(e, carry):
        gate_up(e)
        return carry

    lax.fori_loop(0, n_exp, far_gate_up, 0)
    for part in (A, B):
        down(half, part)
        give_back(far[::-1], (part,))

    sh_acc[...] = jnp.zeros_like(sh_acc)

    def shared_step(i, carry):
        slot = lax.rem(i, n_ring)
        for cp in ring_copies(i, slot):
            cp.wait()
        g = jnp.dot(h_ref[...], ring_g[slot], preferred_element_type=jnp.float32)
        u = jnp.dot(h_ref[...], ring_u[slot], preferred_element_type=jnp.float32)
        a = (jax.nn.silu(g) * u).astype(jnp.bfloat16)
        sh_acc[...] += jnp.dot(a, ring_d[slot], preferred_element_type=jnp.float32)

        @pl.when(i + n_ring < n_steps)
        def _():
            for cp in ring_copies(i + n_ring, slot):
                cp.start()

        return carry

    lax.fori_loop(0, n_steps, shared_step, 0)

    own.wait()

    def returned(k, part):
        for c in ((1 - core,) if k == 0 else (0, 1)):
            pltpu.make_async_remote_copy(
                src_ref=y_buf.at[0, :, cols_of(part)], dst_ref=back.at[k * 2 + c, :, cols_of(part)], send_sem=ret_send.at[0],
                recv_sem=ret_recv.at[(k * 2 + c) * 2 + part[0] // 2], device_id={"ep": partner}, device_id_type=MESH).wait_recv()

    from_near = [slot_of[minus((0, 0), offs[k])] for k in near]
    for k in from_near:
        returned(k, WHOLE)
    n_slot = n_chips * 2 * n_exp * SLOTS_EXP
    for j in range(hidden // 256):
        if j * 256 % (2 * q4) == 0:
            for k in range(n_chips):
                if k not in from_near:
                    returned(k, A if j == 0 else B)
        cs = slice(j * 256, (j + 1) * 256)
        part = lax.dot_general(gate_ref[...], back[:, :, cs].reshape(n_slot, 256), (((0,), (0,)), ((), ())), preferred_element_type=jnp.float32)
        routed = part[:seqs] + part[seqs:2 * seqs] + part[2 * seqs:3 * seqs]
        shared = sh_acc[:, cs].astype(jnp.bfloat16).astype(jnp.float32)
        out_ref[:, cs] = (h_ref[:, cs].astype(jnp.float32) + shared + routed).astype(jnp.bfloat16)
    for cp in sends:
        cp.wait_send()


def slot_tables(n_dev, routes_ref, gates_ref, oh_ref, gate_ref):
    side = int((n_dev // 2) ** 0.5)
    me = lax.axis_index("ep")
    core, my_x, my_y = lax.rem(me, 2), lax.rem(me // 2, side), me // (2 * side)
    top_k, seqs = routes_ref.shape
    per_chip = oh_ref.shape[1] * oh_ref.shape[2] // (n_dev // 2)
    row = lax.broadcasted_iota(jnp.int32, (per_chip, LANES), 0)
    exp_chip = per_chip // SLOTS_EXP
    ids = jnp.concatenate([
        row // SLOTS_EXP + exp_chip * (lax.rem(my_y + dy, side) * side + lax.rem(my_x + dx, side))
        for dx, dy in chip_order(side)], axis=0)
    n_slot = ids.shape[0]
    pos = lax.rem(lax.broadcasted_iota(jnp.int32, (n_slot, LANES), 0), SLOTS_EXP)
    block = lax.broadcasted_iota(jnp.int32, (n_slot, LANES), 1) // seqs
    routes = jnp.concatenate([routes_ref[...]] * (LANES // seqs), axis=1)
    gates = jnp.concatenate([gates_ref[...]] * (LANES // seqs), axis=1)
    has = jnp.zeros((n_slot, LANES), jnp.float32)
    gate = jnp.zeros((n_slot, LANES), jnp.float32)
    for k in range(top_k):
        hit = ids == routes[k:k + 1, :]
        has = jnp.where(hit, 1.0, has)
        gate = jnp.where(hit, gates[k:k + 1, :], gate)
    src = lax.broadcasted_iota(jnp.int32, (LANES, LANES), 0)
    dst = lax.broadcasted_iota(jnp.int32, (LANES, LANES), 1)
    earlier = jnp.where((src < dst) & (src // seqs == dst // seqs), 1.0, 0.0).astype(jnp.bfloat16)
    rank = jnp.dot(has.astype(jnp.bfloat16), earlier, preferred_element_type=jnp.float32)
    sel = jnp.where(rank == pos.astype(jnp.float32), has, 0.0)
    for v in range(2):
        oh_ref[v] = jnp.where(block == 2 * v + core, sel, 0.0).astype(jnp.bfloat16).reshape(oh_ref.shape[1:])
    gate = gate * sel
    g0 = gate.astype(jnp.bfloat16).astype(jnp.float32)
    g1 = (gate - g0).astype(jnp.bfloat16).astype(jnp.float32)
    g2 = gate - g0 - g1
    gate_ref[...] = jnp.where(block == 0, g0, jnp.where(block == 1, g1, jnp.where(block == 2, g2, 0.0))).astype(jnp.bfloat16)


def solution(mesh):
    n_dev = mesh.shape["ep"]

    def device_step(x_blk, cache_blk, len_blk, routes, route_gates, w_q, w_dkv, w_uk, w_uv, w_o, sh_gate, sh_up, sh_down, ex_gate, ex_up, ex_down):
        seqs, hidden = x_blk.shape
        n_exp, _, ff = ex_gate.shape
        n_chips = n_dev // 2
        slots = n_exp * SLOTS_EXP
        half_rows = n_chips * SLOTS_EXP
        bf = jnp.bfloat16
        dma = pltpu.SemaphoreType.DMA
        vmem = pl.BlockSpec(memory_space=pltpu.VMEM)
        hbm = pl.BlockSpec(memory_space=pl.ANY)
        layer_out, kv_row = pl.pallas_call(
            functools.partial(layer_kernel, n_dev),
            out_shape=(jax.ShapeDtypeStruct((seqs, hidden), bf), jax.ShapeDtypeStruct((seqs, w_dkv.shape[1]), bf)),
            in_specs=[vmem, pl.BlockSpec(memory_space=pltpu.SMEM), vmem, vmem] + [hbm] * 12,
            out_specs=(vmem, vmem),
            scratch_shapes=[
                pltpu.VMEM((seqs, hidden), bf),
                pltpu.VMEM((2, n_dev, slots, LANES), bf),
                pltpu.VMEM((n_dev * slots, LANES), bf),
                pltpu.VMEM((n_dev, seqs, hidden), bf),
                pltpu.VMEM((n_dev, slots, LANES), bf),
                pltpu.VMEM((n_exp, half_rows, hidden), bf),
                pltpu.VMEM((n_exp, half_rows, ff), bf),
                pltpu.VMEM((n_dev, slots, hidden), bf),
                pltpu.VMEM((n_dev, slots, hidden), bf),
                pltpu.VMEM((seqs, hidden), jnp.float32),
                dma((64,)), dma((64,)), dma((2 * n_chips,)), dma((2 * n_chips,)),
                dma((n_dev,)), dma((n_dev,)), dma((2 * n_dev,)), dma((2 * n_dev,)), dma,
            ],
            compiler_params=pltpu.CompilerParams(collective_id=0, has_side_effects=True, vmem_limit_bytes=67043328),
        )(x_blk, len_blk, routes.T, route_gates.T, cache_blk.transpose(0, 2, 1), w_q, w_dkv.T, w_uk, w_uv, w_o,
          sh_gate, sh_up, sh_down, ex_gate, ex_up, ex_down)
        return layer_out, kv_row

    batch_spec = P(("dp", "ep"))
    weight_spec = P()
    expert_spec = P("ep")
    in_specs = (batch_spec,) * 5 + (weight_spec,) * 8 + (expert_spec,) * 3
    return jax.shard_map(device_step, mesh=mesh, in_specs=in_specs, out_specs=(batch_spec, batch_spec), check_vma=False)
```
